32 devices in a mesh: tm: 8 (over z, x), space: 4 (over y, core).
Axes of the slice: x: 2, y: 2, z: 4, core: 2. Of those that a mesh axis runs over, the one named last changes fastest.
Arguments:
- checkpoint: float32 [8, 4, 64, 1024], P('tm', None, 'space'), may hold values from -6 to 6
- advect: float32 [8, 2, 64, 1024], P('tm', None, 'space'), may hold values from -0.2 to 0.2
- diffuse: float32 [8, 64, 1024], P('tm', 'space'), may hold values from 0.1 to 0.2
- obs_rows: int32 [8, 8, 8], P('tm', None, 'space'), may hold values from 0 to 1
- obs_values: float32 [8, 8, 8, 4, 8, 1024], P('tm', None, 'space'), may hold values from -6 to 6
- obs_weight: float32 [8], P('tm'), may hold values from 0.5 to 13.5
- error_inverse: float32 [8, 4], P('tm'), may hold values from 0.3 to 3
- rates: float32 [8, 4], replicated, may hold values from 0.07924466 to 1, as said below
Outputs:
- direction: float32 [8, 4, 64, 1024], P('tm', None, 'space')
- grad_rms: float32 [], replicated
The draws below stay inside these ranges and needn't reach their ends.
Inputs may be any that keep to these rules, and one draw needn't show every extreme that they name: `obs_rows`: entry i of the last dimension counts blocks of 8 rows within the rows of space block i // 2; repeats may occur. `rates`: every entry is below 1.
All inputs are finite; a program needn't handle non-finite values.
Results may differ from the reference program's by a relative error of at most 0.0003.
Values sent between devices are 32-bit elements; how exact they have to be, the bound alone decides.
A program may use at most 64 MiB of HBM per device.

```python
import math
import jax
import jax.numpy as jnp
from jax import lax

STATE_COMPONENTS = 4
NX = 1024
ROWS = 16
STEPS = 8
BLOCK = 8
KOBS = 2
SUBWINDOW_COUNT = 8
NY = 64
NOBS = 8


def draw_obs_weight(key, part):
    places = jnp.arange(SUBWINDOW_COUNT, dtype=jnp.float32) / max(SUBWINDOW_COUNT - 1, 1)
    rising = 3.0 ** places
    jitter = jax.random.uniform(key, (SUBWINDOW_COUNT,), jnp.float32, 0.8, 1.2)
    return rising * jitter


def draw_rates(key, part):
    random_key_parts = jax.random.split(jax.random.fold_in(key, 7), 5)
    slow_share = 0.5
    is_slow = jax.random.uniform(random_key_parts[0], (STATE_COMPONENTS,), jnp.float32) < slow_share
    slow_strength = jax.random.uniform(random_key_parts[1], (STATE_COMPONENTS,), jnp.float32, 0.15, 0.4)
    fast_strength = jax.random.uniform(random_key_parts[1], (STATE_COMPONENTS,), jnp.float32, 2.0, 4.0)
    strength = jnp.where(is_slow, slow_strength, fast_strength)
    factor = jnp.exp(jax.random.uniform(random_key_parts[2], (SUBWINDOW_COUNT, STATE_COMPONENTS), jnp.float32, jnp.log(0.6), jnp.log(1.6)))
    logarithm_rate = jnp.log(0.1) * strength[None, :] * factor / SUBWINDOW_COUNT
    surge_location = jax.random.randint(random_key_parts[3], (2, STATE_COMPONENTS), 0, SUBWINDOW_COUNT)
    inside_surge = jnp.any(jnp.arange(SUBWINDOW_COUNT)[:, None, None] == surge_location[None, :, :], axis=1)
    reduction_factor = jax.random.uniform(random_key_parts[4], (SUBWINDOW_COUNT, STATE_COMPONENTS), jnp.float32, 0.5, 0.8)
    return jnp.exp(logarithm_rate) * jnp.where(inside_surge, reduction_factor, 1.0)


def with_ends(entries, stream_key, smallest, largest):
    longest = entries.shape.index(max(entries.shape))
    spots = []
    for shift in (0, 1):
        where = [jax.random.randint(jax.random.fold_in(stream_key, axis), (), 0, length) for axis, length in enumerate(entries.shape)]
        where[longest] = (where[longest] + shift) % entries.shape[longest]
        spots.append(tuple(where))
    return entries.at[spots[0]].set(smallest).at[spots[1]].set(largest)


def steps_of(key, shape, cuts, smallest, largest):
    gain = 1.0
    for position, parts in cuts:
        heights = jax.random.uniform(jax.random.fold_in(jax.random.fold_in(key, 6), position), (parts,), jnp.float32, smallest / len(cuts), largest / len(cuts))
        gain = gain * jnp.repeat(jnp.exp(heights), shape[position] // parts).reshape((-1,) + (1,) * (len(shape) - 1 - position))
    return gain


def gaussian(stream_key, dims, deviation, limit, cuts=(), held_as=jnp.bfloat16):
    drawn = jax.random.normal(stream_key, dims, jnp.float32) * deviation
    if len(cuts) > 0:
        drawn = steps_of(stream_key, dims, cuts, -0.22, 0.18) * drawn
    return jnp.clip(drawn, min=-limit, max=limit).astype(held_as)


def setup_inputs(seed: int = 0) -> dict:
    keys = jax.random.split(jax.random.key(seed), 9)
    checkpoint = gaussian(keys[0], (SUBWINDOW_COUNT, STATE_COMPONENTS, NY, NX), 1.0, 6.0, ((0, 8), (2, 4)), jnp.float32)
    advect = jnp.clip(jax.random.uniform(keys[1], (SUBWINDOW_COUNT, 2, NY, NX), jnp.float32, -0.2, 0.2) * steps_of(keys[1], (SUBWINDOW_COUNT, 2, NY, NX), ((0, 8), (2, 4)), -0.4, 0.0), -0.2, 0.2)
    diffuse = jnp.clip(0.1 + 0.1 * jax.random.uniform(keys[2], (SUBWINDOW_COUNT, NY, NX), jnp.float32) ** steps_of(keys[2], (SUBWINDOW_COUNT, NY, NX), ((0, 8), (1, 4)), -0.2, 0.2), 0.1, 0.2)
    obs_rows = with_ends(jax.random.randint(keys[3], (SUBWINDOW_COUNT, STEPS, NOBS), 0, ROWS // BLOCK), jax.random.fold_in(keys[3], 1), 0, (ROWS // BLOCK) - 1).astype(jnp.int32)
    obs_values = gaussian(keys[4], (SUBWINDOW_COUNT, STEPS, NOBS, STATE_COMPONENTS, BLOCK, NX), 1.0, 6.0, ((0, 8), (2, 4)), jnp.float32)
    obs_weight = draw_obs_weight(jax.random.fold_in(keys[8], 71), 0)
    error_inverse = jnp.clip(jnp.exp(math.log(3.0) - 2.3025851 * jax.random.uniform(keys[6], (SUBWINDOW_COUNT, STATE_COMPONENTS), jnp.float32) ** steps_of(keys[6], (SUBWINDOW_COUNT, STATE_COMPONENTS), ((0, 8),), -0.2, 0.2)), 0.3, 3.0)
    rates = draw_rates(jax.random.fold_in(keys[8], 71), 0)
    return {"checkpoint": checkpoint, "advect": advect, "diffuse": diffuse, "obs_rows": obs_rows, "obs_values": obs_values, "obs_weight": obs_weight, "error_inverse": error_inverse, "rates": rates}


def weights_of(advect_one, diffuse_one):
    centre = 1.0 - 4.0 * diffuse_one
    to_east = diffuse_one - 0.5 * advect_one[0]
    to_west = diffuse_one + 0.5 * advect_one[0]
    to_north = diffuse_one - 0.5 * advect_one[1]
    to_south = diffuse_one + 0.5 * advect_one[1]
    return (centre, to_east, to_west, to_north, to_south)

def pad_rows(values_in):
    return jnp.pad(values_in, ((0, 0), (1, 1), (0, 0)))

def advance(field_now, stencil):
    centre, to_east, to_west, to_north, to_south = stencil
    padded = pad_rows(field_now)
    return centre * field_now + to_east * jnp.roll(field_now, -1, axis=2) + to_west * jnp.roll(field_now, 1, axis=2) + to_north * padded[:, 2:] + to_south * padded[:, :-2]

def retreat(costate, stencil):
    centre, to_east, to_west, to_north, to_south = stencil
    north_flux = pad_rows(to_north * costate)
    south_flux = pad_rows(to_south * costate)
    return centre * costate + jnp.roll(to_east * costate, 1, axis=2) + jnp.roll(to_west * costate, -1, axis=2) + north_flux[:, :-2] + south_flux[:, 2:]

def row_index(rows_step):
    first_rows = jnp.arange(NOBS, dtype=jnp.int32) // KOBS * ROWS + rows_step.astype(jnp.int32) * BLOCK
    return first_rows[:, None] + jnp.arange(BLOCK, dtype=jnp.int32)[None, :]

def observe(field_now, row_picks):
    return jnp.transpose(field_now[:, row_picks], (1, 0, 2, 3))

def spread(misfit, row_picks):
    empty_field = jnp.zeros((STATE_COMPONENTS, NY, NX), jnp.float32)
    return empty_field.at[:, row_picks].add(jnp.transpose(misfit, (1, 0, 2, 3)))

def sweep_forward(packed):
    initial, advect_one, diffuse_one, rows_one, values_one = packed
    stencil = weights_of(advect_one, diffuse_one)
    field_now = initial
    misfits = []
    for moment in range(STEPS):
        field_now = advance(field_now, stencil)
        misfits.append(observe(field_now, row_index(rows_one[moment])) - values_one[moment])
    return (field_now, jnp.stack(misfits))

def sweep_back(packed):
    advect_one, diffuse_one, rows_one, misfit_one, obs_scale, next_term, own_term = packed
    stencil = weights_of(advect_one, diffuse_one)
    costate = spread(obs_scale * misfit_one[STEPS - 1], row_index(rows_one[STEPS - 1])) - next_term
    for moment in range(STEPS, 0, -1):
        costate = retreat(costate, stencil)
        if moment >= 2:
            costate = costate + spread(obs_scale * misfit_one[moment - 2], row_index(rows_one[moment - 2]))
    return costate + own_term

def forward_carry(running, packed):
    rate_row, inno_row, grad_one = packed
    updated = rate_row[:, None, None] * running + inno_row[:, None, None] * grad_one
    return (updated, updated)

def backward_carry(running, packed):
    rate_row, inno_row, forward_one = packed
    updated = inno_row[:, None, None] * forward_one + rate_row[:, None, None] * running
    return (updated, updated)

def reference(checkpoint, advect, diffuse, obs_rows, obs_values, obs_weight, error_inverse, rates):
    end_states, misfits = lax.map(sweep_forward, (checkpoint, advect, diffuse, obs_rows, obs_values))
    prior_end = jnp.concatenate([jnp.zeros_like(end_states[:1]), end_states[:-1]], axis=0)
    forcing = checkpoint - prior_end
    weighted = error_inverse[:, :, None, None] * forcing
    next_term = jnp.concatenate([weighted[1:], jnp.zeros_like(weighted[:1])], axis=0)
    gradient = lax.map(sweep_back, (advect, diffuse, obs_rows, misfits, obs_weight, next_term, weighted))
    square_sum = jnp.sum(gradient * gradient)
    rms_value = jnp.sqrt(square_sum / (SUBWINDOW_COUNT * STATE_COMPONENTS * NY * NX) + 1e-06)
    innovation = jnp.sqrt(1.0 - rates * rates)
    next_rates = jnp.concatenate([rates[1:], jnp.zeros((1, STATE_COMPONENTS), jnp.float32)], axis=0)
    zero_field = jnp.zeros((STATE_COMPONENTS, NY, NX), jnp.float32)
    _, smoothed = lax.scan(forward_carry, zero_field, (rates, innovation, gradient))
    _, result = lax.scan(backward_carry, zero_field, (next_rates, innovation, smoothed), reverse=True)
    return (result / rms_value, rms_value)
```

```python
import functools

import jax
import jax.numpy as jnp
from jax import lax
from jax.experimental import pallas as pl
from jax.experimental.pallas import tpu as pltpu
from jax.sharding import PartitionSpec as P

MESH = pl.DeviceIdType.MESH
LANES = 128
SUB = 8


def mark(name):
    return jax.named_scope(name)


def forcing_spans(steps):
    spans = []
    last = steps - 1
    while last > 0:
        first = max(last - 2, 0)
        spans.append((first, last, last))
        last = first
    return spans


def kernel(
    tm,
    space,
    group,
    rows_hbm,
    weight_hbm,
    einv_hbm,
    rates_hbm,
    ck_hbm,
    adv_hbm,
    dif_hbm,
    obs_hbm,
    out_ref,
    rms_ref,
    rows_smem,
    weight_smem,
    einv_smem,
    rates_smem,
    start,
    fin,
    va,
    vb,
    adv,
    dif,
    cf,
    obs,
    fo,
    nck,
    nei,
    wout,
    wbuf,
    gout,
    gbuf,
    keep,
    aggs,
    lows,
    dout,
    rbuf,
    tab,
    gtab,
    part,
    part_all,
    load_sem,
    y_send,
    f_send,
    halo_recv,
    ck_recv,
    fo_recv,
    edge_send,
    edge_recv,
    w_send,
    w_recv,
    g_send,
    g_recv,
    agg_send,
    agg_recv,
    low_send,
    low_recv,
    ret_send,
    ret_recv,
    sum_send,
    sum_recv,
):
    comps, tiles, nk = ck_hbm.shape[:3]
    rows = tiles * SUB
    steps, kobs = obs_hbm.shape[:2]
    halo = steps
    lo = SUB
    wide = rows + 2 * halo
    own0 = lo + halo
    ngroups = tm // group
    nb = nk // group
    piece = (nb * tiles, SUB, LANES)
    me = lax.axis_index("tm")
    sp = lax.axis_index("space")
    gid = me // group
    mi = lax.rem(me, group)
    own = pl.ds(own0, rows)
    across_all = tm * space
    flat = me * space + sp
    pairs = [(c, min(c + 2, comps)) for c in range(0, comps, 2)]

    def send(src, dst, ssem, rsem, target, guard=None):
        copy = pltpu.make_async_remote_copy(
            src_ref=src, dst_ref=dst, send_sem=ssem, recv_sem=rsem,
            device_id=target, device_id_type=MESH,
        )
        if guard is None:
            copy.start()
        else:
            pl.when(guard)(copy.start)

    def all_of(ref, sem, sent=False, guard=None):
        copy = pltpu.make_async_remote_copy(
            src_ref=ref, dst_ref=ref, send_sem=sem, recv_sem=sem,
            device_id={"tm": lax.rem(me + 1, tm)}, device_id_type=MESH,
        )
        wait = copy.wait_send if sent else copy.wait_recv
        if guard is None:
            wait()
        else:
            pl.when(guard)(wait)

    has_north = sp < space - 1
    has_south = sp > 0
    north = {"space": jnp.minimum(sp + 1, space - 1)}
    south = {"space": jnp.maximum(sp - 1, 0)}
    has_next = me < tm - 1
    has_prev = me > 0
    prv = {"tm": jnp.maximum(me - 1, 0)}

    barrier = pltpu.get_barrier_semaphore()
    for o in range(1, across_all):
        other = lax.rem(flat + o, across_all)
        pl.semaphore_signal(
            barrier, inc=1, device_id={"tm": other // space, "space": lax.rem(other, space)},
            device_id_type=MESH,
        )

    for b in range(tiles):
        at = pl.ds(own0 + SUB * b, SUB)
        pltpu.make_async_copy(dif_hbm.at[b], dif.at[:, at], load_sem.at[0]).start()
        pltpu.make_async_copy(adv_hbm.at[:, b], adv.at[:, :, at], load_sem.at[1]).start()
        pltpu.make_async_copy(ck_hbm.at[:, b], start.at[:, :, at], load_sem.at[2]).start()
    loads = [
        pltpu.make_async_copy(source, target, load_sem.at[3 + k])
        for k, (source, target) in enumerate(
            [
                (einv_hbm, einv_smem),
                (rates_hbm, rates_smem),
                (rows_hbm, rows_smem),
                (weight_hbm, weight_smem),
            ]
            + [(obs_hbm.at[:, :, c0:c1], obs.at[:, :, c0:c1]) for c0, c1 in pairs]
        )
    ]
    small = 4
    for load in loads:
        load.start()

    def clear(first):
        blank = jnp.zeros((nk, halo, LANES), jnp.float32)
        at = slice(first, first + halo)
        dif[:, at] = blank
        for a in range(2):
            adv[a, :, at] = blank
        for c in range(comps):
            start[c, :, at] = blank

            @pl.loop(0, steps)
            def _(t):
                fo[c, t, :, at] = blank

    @pl.when(jnp.logical_not(has_south))
    def _():
        clear(lo)

    @pl.when(jnp.logical_not(has_north))
    def _():
        clear(own0 + rows)

    @pl.when(jnp.logical_not(has_next))
    def _():
        nck[...] = jnp.zeros_like(nck)
        nei[...] = jnp.zeros_like(nei)

    @pl.when(gid == 0)
    def _():
        for c in range(comps):
            wbuf[c, 0] = jnp.zeros((nb, rows, LANES), jnp.float32)

    with mark("loads"):
        pltpu.make_async_copy(dif.at[:, own], dif.at[:, own], load_sem.at[0]).wait()
        pltpu.make_async_copy(adv.at[:, :, own], adv.at[:, :, own], load_sem.at[1]).wait()
        pltpu.make_async_copy(start.at[:, :, own], start.at[:, :, own], load_sem.at[2]).wait()
        for load in loads[:small]:
            load.wait()
    for c in range(comps):
        part[0, c : c + 1, :] = jnp.full((1, LANES), einv_smem[0, c], jnp.float32)
    with mark("barrier"):
        pl.semaphore_wait(barrier, across_all - 1)

    def both_ways(lead, ref, depth, ssem, rsem):
        send(
            ref.at[lead + (pl.ds(own0 + rows - depth, depth),)],
            ref.at[lead + (pl.ds(own0 - depth, depth),)],
            ssem.at[0], rsem.at[0], north, has_north,
        )
        send(
            ref.at[lead + (pl.ds(own0, depth),)],
            ref.at[lead + (pl.ds(own0 + rows, depth),)],
            ssem.at[1], rsem.at[1], south, has_south,
        )

    def both_landed(ref, rsem):
        all_of(ref, rsem.at[0], guard=has_south)
        all_of(ref, rsem.at[1], guard=has_north)

    every = slice(None)
    both_ways((every,), dif, halo, y_send, halo_recv)
    both_ways((every, every), adv, halo, y_send, halo_recv)
    send(part.at[0], nei, edge_send.at[0], edge_recv.at[0], prv, has_prev)
    for n, (c0, c1) in enumerate(pairs):
        both_ways((slice(c0, c1), every), start, halo, y_send, ck_recv.at[n])
        send(
            start.at[c0:c1, :, own], nck.at[c0:c1],
            edge_send.at[1], edge_recv.at[1 + n], prv, has_prev,
        )

    def splat(value):
        return jnp.full((SUB, LANES), value, jnp.float32)

    with mark("tables"):
        for c in range(comps):
            keeps, gains = [], []
            for i in range(group):
                r = splat(rates_smem[c, gid * group + i])
                keeps.append(r)
                gains.append(jnp.sqrt(1.0 - r * r))
            after = splat(rates_smem[c, jnp.minimum(gid * group + group, tm - 1)])
            reach = []
            for i in range(group):
                reach.append(keeps[0] if i == 0 else reach[-1] * keeps[i])
            fwd_gain, back_gain = None, after
            for i in range(group - 1, -1, -1):
                if i < group - 1:
                    fwd_gain = gains[i] * reach[i] + keeps[i + 1] * fwd_gain
                    back_gain = keeps[i + 1] * back_gain
                else:
                    fwd_gain = gains[i] * reach[i]
                tab[c, 0, i] = keeps[i]
                tab[c, 1, i] = gains[i]
                tab[c, 2, i] = fwd_gain
                tab[c, 3, i] = back_gain
            for h in range(ngroups):
                total = None
                fwd_gain, back_gain = None, None
                reach = []
                keeps = [splat(rates_smem[c, h * group + i]) for i in range(group)]
                for i in range(group):
                    reach.append(keeps[0] if i == 0 else reach[-1] * keeps[i])
                back_gain = splat(rates_smem[c, min(h * group + group, tm - 1)])
                for i in range(group - 1, -1, -1):
                    here = jnp.sqrt(1.0 - keeps[i] * keeps[i]) * reach[i]
                    if i < group - 1:
                        fwd_gain = here + keeps[i + 1] * fwd_gain
                        back_gain = keeps[i + 1] * back_gain
                    else:
                        fwd_gain = here
                gtab[c, 0, h] = reach[-1]
                gtab[c, 1, h] = fwd_gain
                gtab[c, 2, h] = back_gain

    lane = lax.broadcasted_iota(jnp.int32, (wide, LANES), 1)
    at_first = lane == 0
    at_last = lane == LANES - 1

    with mark("halos"):
        both_landed(cf.at[0:3, :, 0:halo], halo_recv)
    with mark("coefs"):
        at = slice(lo, lo + wide)
        easts, wests = [], []
        for k in range(nk):
            d, a0, a1 = dif[k, at], adv[0, k, at], adv[1, k, at]
            cf[0, k, at] = 1.0 - 4.0 * d
            easts.append(d - 0.5 * a0)
            wests.append(d + 0.5 * a0)
            cf[1, k, at] = easts[k]
            cf[2, k, at] = wests[k]
            cf[3, k, at] = d - 0.5 * a1
            cf[4, k, at] = d + 0.5 * a1
        for k in range(nk):
            up = pltpu.roll(wests[k], LANES - 1, 1)
            cf[5, k, at] = jnp.where(at_last, pltpu.roll(wests[(k + 1) % nk], LANES - 1, 1), up)
            down = pltpu.roll(easts[k], 1, 1)
            cf[6, k, at] = jnp.where(at_first, pltpu.roll(easts[(k - 1) % nk], 1, 1), down)

    def sweep(srcs, first, count, adjoint):
        at = slice(first, first + count)
        above = slice(first + 1, first + 1 + count)
        below = slice(first - 1, first - 1 + count)
        begin, end = at_first[:count], at_last[:count]
        blocks = {}

        def read(k):
            k %= nk
            if k not in blocks:
                mids = [src[k, at] for src in srcs]
                ups = [pltpu.roll(m, LANES - 1, 1) for m in mids]
                downs = [pltpu.roll(m, 1, 1) for m in mids]
                blocks[k] = (mids, ups, downs)
            return blocks[k]

        read(nk - 1)
        read(0)
        for k in range(nk):
            mids, ups, downs = read(k)
            ups_next, downs_last = read(k + 1)[1], read(k - 1)[2]
            if adjoint:
                weights = (cf[0, k, at], cf[5, k, at], cf[6, k, at], cf[4, k, above], cf[3, k, below])
            else:
                weights = (cf[0, k, at], cf[1, k, at], cf[2, k, at], cf[3, k, at], cf[4, k, at])
            values = []
            for n, src in enumerate(srcs):
                east = jnp.where(end, ups_next[n], ups[n])
                west = jnp.where(begin, downs_last[n], downs[n])
                values.append(
                    weights[0] * mids[n] + weights[1] * east + weights[2] * west
                    + weights[3] * src[k, above] + weights[4] * src[k, below]
                )
            yield k, values

    weight = weight_smem[0, 0]
    spans = forcing_spans(steps)
    depths = sum((last - first) * depth for first, last, depth in spans) + steps

    def forward(n):
        c0, c1 = pairs[n]
        with mark(f"fw{n}"):
            with mark(f"fw{n}w"):
                both_landed(start.at[c0:c1, :, 0:halo], ck_recv.at[n])
                loads[small + n].wait()

            def step(t, srcs, dsts):
                picks = [
                    [jnp.where(rows_smem[i, t] == b, weight, 0.0) for i in range(kobs)]
                    for b in range(tiles)
                ]
                for k, values in sweep(srcs, lo, wide, False):
                    for c, dst, value in zip(range(c0, c1), dsts, values):
                        dst[k, lo : lo + wide] = value
                        seen = [obs[t, i, c, :, k * LANES : (k + 1) * LANES] for i in range(kobs)]
                        for b in range(tiles):
                            total = picks[b][0]
                            pulled = picks[b][0] * seen[0]
                            for i in range(1, kobs):
                                total = total + picks[b][i]
                                pulled = pulled + picks[b][i] * seen[i]
                            r = halo + SUB * b
                            fo[c, t, k, lo + r : lo + r + SUB] = total * value[r : r + SUB] - pulled

            one = [va.at[c - c0] for c in range(c0, c1)]
            two = [vb.at[c - c0] for c in range(c0, c1)]
            step(0, [start.at[c] for c in range(c0, c1)], one)

            @pl.loop(0, steps // 2 - 1)
            def _(p):
                step(2 * p + 1, one, two)
                step(2 * p + 2, two, one)

            step(steps - 1, one, [fin.at[c] for c in range(c0, c1)])
            for first, last, depth in spans:
                at = pl.ds(first, last - first)
                both_ways((slice(c0, c1), at, every), fo, depth, f_send, fo_recv.at[n])

    far = jnp.where(mi == group - 1, gid + 1, gid)
    at_end = mi == group - 1

    def last_forcing(n):
        c0, c1 = pairs[n]
        with mark(f"lf{n}"):
            with mark(f"lf{n}w"):
                if n == 0:
                    all_of(nei, edge_recv.at[0], guard=has_next)
                all_of(nck.at[c0:c1], edge_recv.at[1 + n], guard=has_next)
            for c in range(c0, c1):
                scale = jnp.broadcast_to(nei[c : c + 1, :], (rows, LANES))
                for k in range(nk):
                    w = scale * (nck[c, k] - fin[c, k, own])
                    fo[c, steps - 1, k, own] = fo[c, steps - 1, k, own] - w
                    wout[c, k] = w
            both_ways((slice(c0, c1), steps - 1, every), fo, steps, f_send, fo_recv.at[n])
            for c in range(c0, c1):
                for o in range(group):
                    q = lax.rem(mi + 1 + o, group)
                    outside = o == group - 1
                    send(
                        wout.at[c, pl.ds(q * nb, nb)], wbuf.at[c, lax.rem(mi + 1, group)],
                        w_send.at[1 if outside else 0], w_recv.at[c, jnp.where(at_end, 0, 1)],
                        {"tm": jnp.minimum(far * group + q, tm - 1)},
                        jnp.logical_and(has_next, at_end) if outside else has_next,
                    )

                @pl.when(mi < group - 1)
                def _():
                    wbuf[c, lax.rem(mi + 1, group)] = wout[c, pl.ds(mi * nb, nb)]

    def adjoint(n):
        c0, c1 = pairs[n]
        with mark(f"ad{n}"):
            with mark(f"ad{n}w"):
                both_landed(fo.at[c0:c1, 0, :, 0:depths], fo_recv.at[n])

            def step(m, srcs, dsts):
                for k, values in sweep(srcs, lo, wide, True):
                    for c, dst, value in zip(range(c0, c1), dsts, values):
                        dst[k, lo : lo + wide] = fo[c, m, k, lo : lo + wide] + value

            one = [va.at[c - c0] for c in range(c0, c1)]
            two = [vb.at[c - c0] for c in range(c0, c1)]
            step(steps - 2, [fo.at[c, steps - 1] for c in range(c0, c1)], one)

            @pl.loop(0, steps // 2 - 1)
            def _(p):
                step(steps - 3 - 2 * p, one, two)
                step(steps - 4 - 2 * p, two, one)

            scales = [jnp.where(me == 0, einv_smem[0, c], 0.0) for c in range(c0, c1)]
            for k, values in sweep(one, own0, rows, True):
                for c, scale, value in zip(range(c0, c1), scales, values):
                    gout[c, k] = value + scale * start[c, k, own]
            for c in range(c0, c1):
                for o in range(1, group):
                    q = lax.rem(mi + o, group)
                    send(
                        gout.at[c, pl.ds(q * nb, nb)], gbuf.at[c, mi],
                        g_send.at[0], g_recv.at[c], {"tm": gid * group + q},
                    )
                gbuf[c, mi] = gout[c, pl.ds(mi * nb, nb)]

    def gather(c, squares):
        with mark(f"ga{c}"):
            with mark(f"ga{c}w"):
                all_of(gbuf.at[c, 0 : group - 1], g_recv.at[c])
                all_of(wbuf.at[c, 0], w_recv.at[c, 0], guard=gid > 0)
                all_of(wbuf.at[c, 0 : group - 1], w_recv.at[c, 1], guard=at_end)
                if group > 2:
                    all_of(
                        wbuf.at[c, 0 : group - 2], w_recv.at[c, 1],
                        guard=jnp.logical_not(at_end),
                    )
            run, ahead = None, []
            for i in range(group):
                g = gbuf[c, i].reshape(piece) + wbuf[c, i].reshape(piece)
                squares = squares + jnp.sum(g * g, axis=0)
                run = tab[c, 1, i] * g if i == 0 else tab[c, 0, i] * run + tab[c, 1, i] * g
                ahead.append(run)
            aggs[c, gid] = run.reshape(aggs.shape[2:])
            for i in range(group - 1, -1, -1):
                here = tab[c, 1, i] * ahead[i]
                run = here if i == group - 1 else here + tab[c, 0, i + 1] * run
                keep[c, i] = run
            lows[c, gid] = run.reshape(lows.shape[2:])
            for o in range(1, ngroups):
                to = lax.rem(gid + o, ngroups)
                target = {"tm": to * group + mi}
                send(
                    aggs.at[c, gid], aggs.at[c, gid], agg_send.at[o], agg_recv.at[c, o],
                    target, jnp.logical_or(to > gid, gid < ngroups - 1),
                )
                send(
                    lows.at[c, gid], lows.at[c, gid], low_send.at[o], low_recv.at[c, o],
                    target, to < gid,
                )
            return squares


    def spread(c):
        with mark(f"sp{c}"):
            with mark(f"sp{c}w"):
                for o in range(1, ngroups):
                    come = lax.rem(gid + ngroups - o, ngroups)
                    all_of(
                        aggs.at[c, 0], agg_recv.at[c, o],
                        guard=jnp.logical_or(gid > come, come < ngroups - 1),
                    )
                    all_of(lows.at[c, 0], low_recv.at[c, o], guard=gid < come)
            zero = jnp.zeros(piece, jnp.float32)
            carried = [zero]
            for h in range(ngroups - 1):
                a = aggs[c, h].reshape(piece)
                carried.append(a if h == 0 else gtab[c, 0, h] * carried[h] + a)
            before, behind = zero, zero
            run = None
            for h in range(ngroups - 1, 0, -1):
                here = lows[c, h].reshape(piece) + gtab[c, 1, h] * carried[h]
                run = here if run is None else here + gtab[c, 2, h] * run
                before = jnp.where(gid == h, carried[h], before)
                behind = jnp.where(gid == h - 1, run, behind)
            for i in range(group):
                value = keep[c, i] + tab[c, 2, i] * before + tab[c, 3, i] * behind
                dout[c, i] = value.reshape(dout.shape[2:])
            for o in range(1, group):
                q = lax.rem(mi + o, group)
                send(
                    dout.at[c, q], rbuf.at[c, pl.ds(mi * nb, nb)],
                    ret_send.at[0], ret_recv.at[c], {"tm": gid * group + q},
                )
            rbuf[c, pl.ds(mi * nb, nb)] = dout[c, mi]

    squares = jnp.zeros((SUB, LANES), jnp.float32)
    for n in range(len(pairs)):
        forward(n)
    for n in range(len(pairs)):
        last_forcing(n)
    for n in range(len(pairs)):
        adjoint(n)
    for c in range(comps):
        squares = gather(c, squares)
    mine = jnp.sum(squares, axis=0, keepdims=True)
    part_all[flat] = mine
    for o in range(1, across_all):
        other = lax.rem(flat + o, across_all)
        send(
            part_all.at[flat], part_all.at[flat], sum_send.at[0], sum_recv.at[0],
            {"tm": other // space, "space": lax.rem(other, space)},
        )
    for c in range(comps):
        spread(c)

    with mark("sums"):
        all_of(part_all.at[0 : across_all - 1], sum_recv.at[0])
    total = jnp.sum(part_all[...], axis=0)
    entries = across_all * comps * rows * nk * LANES
    rms = jnp.sqrt(jnp.sum(total, axis=(0, 1), keepdims=True) / entries + 1e-06)
    rms_ref[...] = rms
    inverse = jnp.broadcast_to(1.0 / rms, (SUB, LANES))
    for c in range(comps):
        with mark(f"out{c}"):
            with mark(f"out{c}w"):
                all_of(dout.at[c, 0 : group - 1], ret_recv.at[c])
            for k in range(nk):
                for b in range(tiles):
                    at = slice(SUB * b, SUB * (b + 1))
                    out_ref[0, c, at, k * LANES : (k + 1) * LANES] = rbuf[c, k, at] * inverse
    with mark("ends"):
        for d, guard in ((0, has_north), (1, has_south)):
            all_of(cf.at[0 : 3 + comps, :, 0:halo], y_send.at[d], True, guard)
            all_of(fo.at[:, 0, :, 0:depths], f_send.at[d], True, guard)
        all_of(part.at[0], edge_send.at[0], True, has_prev)
        all_of(nck, edge_send.at[1], True, has_prev)
        all_of(wbuf.at[:, 0 : group - 1], w_send.at[0], True, has_next)
        all_of(wbuf.at[:, 0], w_send.at[1], True, jnp.logical_and(has_next, at_end))
        all_of(gbuf.at[:, 0 : group - 1], g_send.at[0], True)
        for o in range(1, ngroups):
            to = lax.rem(gid + o, ngroups)
            all_of(
                aggs.at[:, 0], agg_send.at[o], True,
                jnp.logical_or(to > gid, gid < ngroups - 1),
            )
            all_of(lows.at[:, 0], low_send.at[o], True, to < gid)
        all_of(dout.at[:, 0 : group - 1], ret_send.at[0], True)
        all_of(part_all.at[0 : across_all - 1], sum_send.at[0], True)


def on_device(tm, space, checkpoint, advect, diffuse, obs_rows, obs_values, obs_weight, error_inverse, rates):
    comps, rows, cols = checkpoint.shape[1:]
    steps, kobs, _, block, _ = obs_values.shape[1:]
    nk = cols // LANES
    tiles = rows // SUB
    group = min(max(tm // 2, 1), nk)
    ngroups = tm // group
    nb = nk // group
    tall = rows + 2 * steps + 2 * SUB
    npairs = -(-comps // 2)
    f32 = jnp.float32
    hbm = pl.BlockSpec(memory_space=pltpu.HBM)
    vmem = pl.BlockSpec(memory_space=pltpu.VMEM)
    dma = pltpu.SemaphoreType.DMA

    def tiled(x):
        lead = x.shape[:-2]
        n = len(lead)
        x = x.reshape(lead + (tiles, SUB, nk, LANES))
        return x.transpose(tuple(range(n)) + (n, n + 2, n + 1, n + 3))

    out, rms = pl.pallas_call(
        functools.partial(kernel, tm, space, group),
        out_shape=(
            pltpu.VMEM((1, comps, rows, cols), f32),
            pltpu.VMEM((1, 1), f32),
        ),
        in_specs=[hbm] * 8,
        out_specs=(vmem, vmem),
        scratch_shapes=[
            pltpu.SMEM((kobs, steps), jnp.int32),
            pltpu.SMEM((1, 1), f32),
            pltpu.SMEM((1, comps), f32),
            pltpu.SMEM((comps, tm), f32),
            pltpu.VMEM((comps, nk, tall, LANES), f32),
            pltpu.VMEM((comps, nk, tall, LANES), f32),
            pltpu.VMEM((2, nk, tall, LANES), f32),
            pltpu.VMEM((2, nk, tall, LANES), f32),
            pltpu.VMEM((2, nk, tall, LANES), f32),
            pltpu.VMEM((nk, tall, LANES), f32),
            pltpu.VMEM((7, nk, tall, LANES), f32),
            pltpu.VMEM((steps, kobs, comps, block, cols), f32),
            pltpu.VMEM((comps, steps, nk, tall, LANES), f32),
            pltpu.VMEM((comps, nk, rows, LANES), f32),
            pltpu.VMEM((SUB, LANES), f32),
            pltpu.VMEM((comps, nk, rows, LANES), f32),
            pltpu.VMEM((comps, group, nb, rows, LANES), f32),
            pltpu.VMEM((comps, nk, rows, LANES), f32),
            pltpu.VMEM((comps, group, nb, rows, LANES), f32),
            pltpu.VMEM((comps, group, nb * tiles, SUB, LANES), f32),
            pltpu.VMEM((comps, ngroups, nb, rows, LANES), f32),
            pltpu.VMEM((comps, ngroups, nb, rows, LANES), f32),
            pltpu.VMEM((comps, group, nb, rows, LANES), f32),
            pltpu.VMEM((comps, nk, rows, LANES), f32),
            pltpu.VMEM((comps, 4, group, SUB, LANES), f32),
            pltpu.VMEM((comps, 3, ngroups, SUB, LANES), f32),
            pltpu.VMEM((1, SUB, LANES), f32),
            pltpu.VMEM((tm * space, 1, LANES), f32),
            dma((7 + npairs,)),
            dma((2,)),
            dma((2,)),
            dma((2,)),
            dma((npairs, 2)),
            dma((npairs, 2)),
            dma((2,)),
            dma((1 + npairs,)),
            dma((2,)),
            dma((comps, 2)),
            dma((1,)),
            dma((comps,)),
            dma((ngroups,)),
            dma((comps, ngroups)),
            dma((ngroups,)),
            dma((comps, ngroups)),
            dma((1,)),
            dma((comps,)),
            dma((1,)),
            dma((1,)),
        ],
        compiler_params=pltpu.CompilerParams(
            collective_id=0, has_side_effects=True, vmem_limit_bytes=60 * 1024 * 1024
        ),
    )(
        obs_rows[0].T, obs_weight.reshape(1, 1), error_inverse, rates.T,
        tiled(checkpoint[0]), tiled(advect[0]), tiled(diffuse[0]), obs_values[0],
    )
    return out, rms.reshape(())


def solution(mesh):
    placed = (
        P("tm", None, "space", None),
        P("tm", None, "space", None),
        P("tm", "space", None),
        P("tm", None, "space"),
        P("tm", None, "space", None, None, None),
        P("tm"),
        P("tm", None),
        P(),
    )
    return jax.shard_map(
        functools.partial(on_device, mesh.shape["tm"], mesh.shape["space"]),
        mesh=mesh,
        in_specs=placed,
        out_specs=(P("tm", None, "space", None), P()),
        check_vma=False,
    )
```

```python
import functools

import jax
import jax.numpy as jnp
from jax import lax
from jax.experimental import pallas as pl
from jax.experimental.pallas import tpu as pltpu
from jax.sharding import PartitionSpec as P

MESH = pl.DeviceIdType.MESH
LANES = 128
SUB = 8


def mark(name):
    return jax.named_scope(name)


def forcing_spans(first, last):
    spans = []
    while last > first:
        begin = max(last - 2, first)
        spans.append((begin, last, last - first))
        last = begin
    return spans


def units_of(comps, steps):
    units = [(0, 2)] + [(c, c + 1) for c in range(2, comps)]
    return units, [steps // 2] * len(units)


def kernel(
    tm,
    space,
    group,
    rows_hbm,
    weight_hbm,
    einv_hbm,
    rates_hbm,
    ck_hbm,
    adv_hbm,
    dif_hbm,
    obs_hbm,
    out_ref,
    rms_ref,
    rows_smem,
    weight_smem,
    einv_smem,
    rates_smem,
    start,
    fin,
    va,
    vb,
    pa,
    pb,
    mid,
    adv,
    dif,
    cf,
    obs,
    fo,
    nck,
    nei,
    wout,
    wbuf,
    gout,
    gbuf,
    keep,
    aggs,
    lows,
    dout,
    rbuf,
    tab,
    gtab,
    part,
    part_all,
    load_sem,
    y_send,
    f_send,
    halo_recv,
    ck_recv,
    fo_recv,
    mid_recv,
    edge_send,
    edge_recv,
    w_send,
    w_recv,
    g_send,
    g_recv,
    agg_send,
    agg_recv,
    low_send,
    low_recv,
    ret_send,
    ret_recv,
    sum_send,
    sum_recv,
):
    comps, tiles, nk = ck_hbm.shape[:3]
    rows = tiles * SUB
    steps, kobs = obs_hbm.shape[:2]
    halo = steps
    lo = SUB
    wide = rows + 2 * halo
    own0 = lo + halo
    ngroups = tm // group
    nb = nk // group
    piece = (nb * tiles, SUB, LANES)
    me = lax.axis_index("tm")
    sp = lax.axis_index("space")
    gid = me // group
    mi = lax.rem(me, group)

    def owner(member, which):
        return lax.rem(member + lax.rem(which, 2) * (group // 2), group)

    part_of = owner(mi, gid)
    own = pl.ds(own0, rows)
    across_all = tm * space
    flat = me * space + sp
    pairs, refetch = units_of(comps, steps)

    def send(src, dst, ssem, rsem, target, guard=None):
        copy = pltpu.make_async_remote_copy(
            src_ref=src, dst_ref=dst, send_sem=ssem, recv_sem=rsem,
            device_id=target, device_id_type=MESH,
        )
        if guard is None:
            copy.start()
        else:
            pl.when(guard)(copy.start)

    def all_of(ref, sem, sent=False, guard=None):
        copy = pltpu.make_async_remote_copy(
            src_ref=ref, dst_ref=ref, send_sem=sem, recv_sem=sem,
            device_id={"tm": lax.rem(me + 1, tm)}, device_id_type=MESH,
        )
        wait = copy.wait_send if sent else copy.wait_recv
        if guard is None:
            wait()
        else:
            pl.when(guard)(wait)

    has_north = sp < space - 1
    has_south = sp > 0
    north = {"space": jnp.minimum(sp + 1, space - 1)}
    south = {"space": jnp.maximum(sp - 1, 0)}
    has_next = me < tm - 1
    has_prev = me > 0
    prv = {"tm": jnp.maximum(me - 1, 0)}

    for b in range(tiles):
        at = pl.ds(own0 + SUB * b, SUB)
        pltpu.make_async_copy(dif_hbm.at[b], dif.at[:, at], load_sem.at[0]).start()
        pltpu.make_async_copy(adv_hbm.at[:, b], adv.at[:, :, at], load_sem.at[1]).start()
        pltpu.make_async_copy(ck_hbm.at[:, b], start.at[:, :, at], load_sem.at[2]).start()
    loads = [
        pltpu.make_async_copy(source, target, load_sem.at[3 + k])
        for k, (source, target) in enumerate(
            [
                (einv_hbm, einv_smem),
                (rates_hbm, rates_smem),
                (rows_hbm, rows_smem),
                (weight_hbm, weight_smem),
            ]
            + [(obs_hbm.at[:, :, c0:c1], obs.at[:, :, c0:c1]) for c0, c1 in pairs]
        )
    ]
    small = 4
    for load in loads:
        load.start()

    barrier = pltpu.get_barrier_semaphore()
    for o in range(1, across_all):
        other = lax.rem(flat + o, across_all)
        pl.semaphore_signal(
            barrier, inc=1, device_id={"tm": other // space, "space": lax.rem(other, space)},
            device_id_type=MESH,
        )

    def clear(first):
        blank = jnp.zeros((nk, halo, LANES), jnp.float32)
        at = slice(first, first + halo)
        dif[:, at] = blank
        for a in range(2):
            adv[a, :, at] = blank
        for c in range(comps):
            start[c, :, at] = blank
            for m in range(steps):
                fo[c, m, :, at] = blank
            side = 0 if first < own0 else SUB
            mid[c, :, side : side + SUB] = jnp.zeros((nk, SUB, LANES), jnp.float32)

    @pl.when(jnp.logical_not(has_south))
    def _():
        clear(lo)

    @pl.when(jnp.logical_not(has_north))
    def _():
        clear(own0 + rows)

    @pl.when(jnp.logical_not(has_next))
    def _():
        nck[...] = jnp.zeros_like(nck)
        nei[...] = jnp.zeros_like(nei)

    @pl.when(gid == 0)
    def _():
        for c in range(comps):
            wbuf[c, 0] = jnp.zeros((nb, rows, LANES), jnp.float32)

    with mark("loads"):
        pltpu.make_async_copy(dif.at[:, own], dif.at[:, own], load_sem.at[0]).wait()
        pltpu.make_async_copy(adv.at[:, :, own], adv.at[:, :, own], load_sem.at[1]).wait()
        pltpu.make_async_copy(start.at[:, :, own], start.at[:, :, own], load_sem.at[2]).wait()
        for load in loads[:small]:
            load.wait()
    for c in range(comps):
        part[0, c : c + 1, :] = jnp.full((1, LANES), einv_smem[0, c], jnp.float32)
    with mark("barrier"):
        pl.semaphore_wait(barrier, across_all - 1)

    def both_ways(lead, ref, depth, ssem, rsem):
        send(
            ref.at[lead + (pl.ds(own0 + rows - depth, depth),)],
            ref.at[lead + (pl.ds(own0 - depth, depth),)],
            ssem.at[0], rsem.at[0], north, has_north,
        )
        send(
            ref.at[lead + (pl.ds(own0, depth),)],
            ref.at[lead + (pl.ds(own0 + rows, depth),)],
            ssem.at[1], rsem.at[1], south, has_south,
        )

    def both_landed(ref, rsem):
        all_of(ref, rsem.at[0], guard=has_south)
        all_of(ref, rsem.at[1], guard=has_north)

    every = slice(None)
    both_ways((every,), dif, halo, y_send, halo_recv)
    both_ways((every, every), adv, halo, y_send, halo_recv)
    send(part.at[0], nei, edge_send.at[0], edge_recv.at[0], prv, has_prev)
    for n, (c0, c1) in enumerate(pairs):
        both_ways((slice(c0, c1), every), start, halo, y_send, ck_recv.at[n])
        send(
            start.at[c0:c1, :, own], nck.at[c0:c1],
            edge_send.at[1], edge_recv.at[1 + n], prv, has_prev,
        )

    def splat(value):
        return jnp.full((SUB, LANES), value, jnp.float32)

    with mark("tables"):
        for c in range(comps):
            keeps, gains = [], []
            for i in range(group):
                r = splat(rates_smem[c, gid * group + i])
                keeps.append(r)
                gains.append(jnp.sqrt(1.0 - r * r))
            after = splat(rates_smem[c, jnp.minimum(gid * group + group, tm - 1)])
            reach = []
            for i in range(group):
                reach.append(keeps[0] if i == 0 else reach[-1] * keeps[i])
            fwd_gain, back_gain = None, after
            for i in range(group - 1, -1, -1):
                if i < group - 1:
                    fwd_gain = gains[i] * reach[i] + keeps[i + 1] * fwd_gain
                    back_gain = keeps[i + 1] * back_gain
                else:
                    fwd_gain = gains[i] * reach[i]
                tab[c, 0, i] = keeps[i]
                tab[c, 1, i] = gains[i]
                tab[c, 2, i] = fwd_gain
                tab[c, 3, i] = back_gain
            for h in range(ngroups):
                total = None
                fwd_gain, back_gain = None, None
                reach = []
                keeps = [splat(rates_smem[c, h * group + i]) for i in range(group)]
                for i in range(group):
                    reach.append(keeps[0] if i == 0 else reach[-1] * keeps[i])
                back_gain = splat(rates_smem[c, min(h * group + group, tm - 1)])
                for i in range(group - 1, -1, -1):
                    here = jnp.sqrt(1.0 - keeps[i] * keeps[i]) * reach[i]
                    if i < group - 1:
                        fwd_gain = here + keeps[i + 1] * fwd_gain
                        back_gain = keeps[i + 1] * back_gain
                    else:
                        fwd_gain = here
                gtab[c, 0, h] = reach[-1]
                gtab[c, 1, h] = fwd_gain
                gtab[c, 2, h] = back_gain

    lane = lax.broadcasted_iota(jnp.int32, (wide, LANES), 1)
    at_first = lane == 0
    at_last = lane == LANES - 1

    def columns(read, dst, at):
        rows_of = at.stop - at.start
        begin, end = at_first[:rows_of], at_last[:rows_of]
        ups, downs = [], []
        for k in range(nk):
            value = read(k)
            ups.append(pltpu.roll(value, LANES - 1, 1))
            downs.append(pltpu.roll(value, 1, 1))
            if k > 0:
                dst[1, k - 1, at] = jnp.where(end, ups[k], ups[k - 1])
                dst[2, k, at] = jnp.where(begin, downs[k - 1], downs[k])
        dst[1, nk - 1, at] = jnp.where(end, ups[0], ups[nk - 1])
        dst[2, 0, at] = jnp.where(begin, downs[nk - 1], downs[0])

    def apply(srcs, k, first, count, adjoint):
        at = slice(first, first + count)
        above = slice(first + 1, first + 1 + count)
        below = slice(first - 1, first - 1 + count)
        if adjoint:
            weights = (cf[0, k, at], cf[5, k, at], cf[6, k, at], cf[4, k, above], cf[3, k, below])
        else:
            weights = (cf[0, k, at], cf[1, k, at], cf[2, k, at], cf[3, k, at], cf[4, k, at])
        return [
            weights[0] * src[0, k, at] + weights[1] * src[1, k, at] + weights[2] * src[2, k, at]
            + weights[3] * src[0, k, above] + weights[4] * src[0, k, below]
            for src in srcs
        ]

    def window(depth):
        pad = -(-2 * depth // SUB) * SUB // 2
        return own0 - pad, rows + 2 * pad

    def step(srcs, dsts, adjoint, adjust, depth, turn):
        first, count = window(depth)
        at = slice(first, first + count)
        begin, end = at_first[:count], at_last[:count]
        ups, downs = {}, {}
        order = [(turn + i) % nk for i in range(nk)]

        def join(west_of, k, n, dst):
            dst[1, west_of, at] = jnp.where(end, ups[k, n], ups[west_of, n])
            dst[2, k, at] = jnp.where(begin, downs[west_of, n], downs[k, n])

        for k in order:
            values = apply(srcs, k, first, count, adjoint)
            for n, dst in enumerate(dsts):
                value = adjust(k, n, at, values[n])
                dst[0, k, at] = value
                ups[k, n] = pltpu.roll(value, LANES - 1, 1)
                downs[k, n] = pltpu.roll(value, 1, 1)
                if k != order[0]:
                    join((k - 1) % nk, k, n, dst)
        for n, dst in enumerate(dsts):
            join(order[-1], order[0], n, dst)

    def beside(source, dst):
        for side, first in ((0, own0 - SUB), (1, own0 + rows)):
            near = slice(first, first + SUB)

            def read(k):
                value = source(side, k, near)
                dst[0, k, near] = value
                return value

            columns(read, dst, near)

    def inside(source, dst):
        mine = slice(own0, own0 + rows)

        def read(k):
            value = source(k, mine)
            dst[0, k, mine] = value
            return value

        columns(read, dst, mine)

    def ready(n):
        c0, c1 = pairs[n]
        for c in range(c0, c1):
            inside(lambda k, mine: start[c, k, mine], va.at[c - c0])

    ready(0)
    with mark("halos"):
        both_landed(cf.at[0:3, :, 0:halo], halo_recv)
    with mark("coefs"):
        at = slice(lo, lo + wide)
        easts, wests = [], []
        for k in range(nk):
            d, a0, a1 = dif[k, at], adv[0, k, at], adv[1, k, at]
            cf[0, k, at] = 1.0 - 4.0 * d
            easts.append(d - 0.5 * a0)
            wests.append(d + 0.5 * a0)
            cf[1, k, at] = easts[k]
            cf[2, k, at] = wests[k]
            cf[3, k, at] = d - 0.5 * a1
            cf[4, k, at] = d + 0.5 * a1
        for k in range(nk):
            up = pltpu.roll(wests[k], LANES - 1, 1)
            cf[5, k, at] = jnp.where(at_last, pltpu.roll(wests[(k + 1) % nk], LANES - 1, 1), up)
            down = pltpu.roll(easts[k], 1, 1)
            cf[6, k, at] = jnp.where(at_first, pltpu.roll(easts[(k - 1) % nk], 1, 1), down)

    weight = weight_smem[0, 0]
    late = [forcing_spans(again, steps - 1) for again in refetch]
    soon = [forcing_spans(0, again - 1) if again > 0 else [] for again in refetch]
    late_rows = [
        sum((last - first) * depth for first, last, depth in spans) + steps - again
        for spans, again in zip(late, refetch)
    ]
    soon_rows = [
        sum((last - first) * depth for first, last, depth in spans) + again
        for spans, again in zip(soon, refetch)
    ]

    def send_forcing(n, spans, rsem):
        c0, c1 = pairs[n]
        for first, last, depth in spans:
            at = pl.ds(first, last - first)
            both_ways((slice(c0, c1), at, every), fo, depth, f_send.at[n], rsem.at[n])

    def forward(n):
        c0, c1 = pairs[n]
        with mark(f"fw{n}"):
            with mark(f"fw{n}w"):
                both_landed(start.at[c0:c1, :, 0:halo], ck_recv.at[n])
                loads[small + n].wait()
            one = [va.at[j] for j in range(c1 - c0)]
            two = [vb.at[j] for j in range(c1 - c0)]
            if n > 0:
                ready(n)
            for c in range(c0, c1):
                beside(lambda side, k, near: start[c, k, near], one[c - c0])

            def watch(t, dsts):
                picks = [
                    [jnp.where(rows_smem[i, t] == b, weight, 0.0) for i in range(kobs)]
                    for b in range(tiles)
                ]

                def compare(k, j, b, value):
                    c = c0 + j
                    lanes = slice(k * LANES, (k + 1) * LANES)
                    total = picks[b][0]
                    pulled = picks[b][0] * obs[t, 0, c, :, lanes]
                    for i in range(1, kobs):
                        total = total + picks[b][i]
                        pulled = pulled + picks[b][i] * obs[t, i, c, :, lanes]
                    r = own0 + SUB * b
                    fo[c, t, k, r : r + SUB] = total * value - pulled

                def adjust(k, j, at, value):
                    for b in range(tiles):
                        r = own0 + SUB * b - at.start
                        if r % SUB == 0:
                            compare(k, j, b, value[r : r + SUB])
                    return value

                def after(at):
                    if (own0 - at.start) % SUB:
                        for k in range(nk):
                            for j, dst in enumerate(dsts):
                                for b in range(tiles):
                                    r = own0 + SUB * b
                                    compare(k, j, b, dst[0, k, r : r + SUB])

                return adjust, after

            def advance(t, srcs, dsts, depth):
                adjust, after = watch(t, dsts)
                step(srcs, dsts, False, adjust, depth, t)
                after(slice(window(depth)[0], None))

            for t in range(steps - 1):
                advance(t, one, two, steps - 1 - t)
                one, two = two, one
            adjust, _ = watch(steps - 1, None)
            own_rows = slice(own0, own0 + rows)
            for k in range(nk):
                for j, value in enumerate(apply(one, k, own0, rows, False)):
                    fin[c0 + j, k, own_rows] = adjust(k, j, own_rows, value)

    far = jnp.where(mi == group - 1, gid + 1, gid)
    at_end = mi == group - 1

    def last_forcing(n):
        c0, c1 = pairs[n]
        with mark(f"lf{n}"):
            with mark(f"lf{n}w"):
                if n == 0:
                    all_of(nei, edge_recv.at[0], guard=has_next)
                all_of(nck.at[c0:c1], edge_recv.at[1 + n], guard=has_next)
            for c in range(c0, c1):
                scale = jnp.broadcast_to(nei[c : c + 1, :], (rows, LANES))
                for k in range(nk):
                    w = scale * (nck[c, k] - fin[c, k, own])
                    fo[c, steps - 1, k, own] = fo[c, steps - 1, k, own] - w
                    wout[c, k] = w
            both_ways(
                (slice(c0, c1), steps - 1, every), fo, steps - refetch[n],
                f_send.at[n], fo_recv.at[n],
            )
            for c in range(c0, c1):
                for o in range(group):
                    t = lax.rem(mi + 1 + o, group)
                    outside = o == group - 1
                    send(
                        wout.at[c, pl.ds(owner(t, far) * nb, nb)], wbuf.at[c, lax.rem(mi + 1, group)],
                        w_send.at[1 if outside else 0], w_recv.at[c, jnp.where(at_end, 0, 1)],
                        {"tm": jnp.minimum(far * group + t, tm - 1)},
                        jnp.logical_and(has_next, at_end) if outside else has_next,
                    )

                @pl.when(mi < group - 1)
                def _():
                    wbuf[c, lax.rem(mi + 1, group)] = wout[c, pl.ds(part_of * nb, nb)]

                inside(lambda k, mine: fo[c, steps - 1, k, mine], pa.at[c])

    def retreat(n, first, last, target, srcs, spare):
        c0, c1 = pairs[n]

        def force(m):
            return lambda k, j, at, value: value + fo[c0 + j, m, k, at]

        for m in range(last, first - 1, -1):
            step(srcs, spare, True, force(m), m - target, steps - m)
            srcs, spare = spare, srcs
        return srcs

    def adjoint(n):
        c0, c1 = pairs[n]
        again = refetch[n]
        with mark(f"ad{n}"):
            with mark(f"ad{n}w"):
                both_landed(fo.at[c0:c1, 0, :, 0 : late_rows[n]], fo_recv.at[n])
            for c in range(c0, c1):
                beside(lambda side, k, near: fo[c, steps - 1, k, near], pa.at[c])
            ends = [pa.at[c] for c in range(c0, c1)]
            spare = [pb.at[c] for c in range(c0, c1)]
            if again == 0:
                return retreat(n, 0, steps - 2, -1, ends, spare)
            ends = retreat(n, again - 1, steps - 2, again - 1, ends, spare)
            for c, end in zip(range(c0, c1), ends):
                send(
                    end.at[0, :, pl.ds(own0 + rows - again, again)],
                    mid.at[c, :, pl.ds(SUB - again, again)],
                    f_send.at[n, 0], mid_recv.at[n, 0], north, has_north,
                )
                send(
                    end.at[0, :, pl.ds(own0, again)], mid.at[c, :, pl.ds(SUB, again)],
                    f_send.at[n, 1], mid_recv.at[n, 1], south, has_south,
                )
            return ends

    def finish(n, one):
        c0, c1 = pairs[n]
        again = refetch[n]
        with mark(f"af{n}"):
            if again > 0:
                with mark(f"af{n}w"):
                    both_landed(fo.at[c0:c1, 0, :, 0 : soon_rows[n]], mid_recv.at[n])
                for c, end in zip(range(c0, c1), one):
                    beside(lambda side, k, near: mid[c, k, SUB * side : SUB * side + SUB], end)
                first = [va.at[j] for j in range(c1 - c0)]
                other = [vb.at[j] for j in range(c1 - c0)]
                retreat(n, again - 2, again - 2, -1, one, first)
                one = retreat(n, 0, again - 3, -1, first, other)
            scales = [jnp.where(me == 0, einv_smem[0, c], 0.0) for c in range(c0, c1)]
            for k in range(nk):
                values = apply(one, k, own0, rows, True)
                for c, scale, value in zip(range(c0, c1), scales, values):
                    gout[c, k] = value + scale * start[c, k, own]
            for c in range(c0, c1):
                for o in range(1, group):
                    q = lax.rem(mi + o, group)
                    send(
                        gout.at[c, pl.ds(owner(q, gid) * nb, nb)], gbuf.at[c, mi],
                        g_send.at[0], g_recv.at[c], {"tm": gid * group + q},
                    )
                gbuf[c, mi] = gout[c, pl.ds(part_of * nb, nb)]

    def gather(c, squares):
        with mark(f"ga{c}"):
            with mark(f"ga{c}w"):
                all_of(gbuf.at[c, 0 : group - 1], g_recv.at[c])
                all_of(wbuf.at[c, 0], w_recv.at[c, 0], guard=gid > 0)
                all_of(wbuf.at[c, 0 : group - 1], w_recv.at[c, 1], guard=at_end)
                if group > 2:
                    all_of(
                        wbuf.at[c, 0 : group - 2], w_recv.at[c, 1],
                        guard=jnp.logical_not(at_end),
                    )
            run, ahead = None, []
            for i in range(group):
                g = gbuf[c, i].reshape(piece) + wbuf[c, i].reshape(piece)
                squares = squares + jnp.sum(g * g, axis=0)
                run = tab[c, 1, i] * g if i == 0 else tab[c, 0, i] * run + tab[c, 1, i] * g
                ahead.append(run)
            aggs[c, gid] = run.reshape(aggs.shape[2:])
            for i in range(group - 1, -1, -1):
                here = tab[c, 1, i] * ahead[i]
                run = here if i == group - 1 else here + tab[c, 0, i + 1] * run
                keep[c, i] = run
            lows[c, gid] = run.reshape(lows.shape[2:])
            for o in range(1, ngroups):
                to = lax.rem(gid + o, ngroups)
                target = {"tm": to * group + owner(part_of, to)}
                send(
                    aggs.at[c, gid], aggs.at[c, gid], agg_send.at[o], agg_recv.at[c, o],
                    target, jnp.logical_or(to > gid, gid < ngroups - 1),
                )
                send(
                    lows.at[c, gid], lows.at[c, gid], low_send.at[o], low_recv.at[c, o],
                    target, to < gid,
                )
            return squares


    def spread(c):
        with mark(f"sp{c}"):
            with mark(f"sp{c}w"):
                for o in range(1, ngroups):
                    come = lax.rem(gid + ngroups - o, ngroups)
                    all_of(
                        aggs.at[c, 0], agg_recv.at[c, o],
                        guard=jnp.logical_or(gid > come, come < ngroups - 1),
                    )
                    all_of(lows.at[c, 0], low_recv.at[c, o], guard=gid < come)
            zero = jnp.zeros(piece, jnp.float32)
            carried = [zero]
            for h in range(ngroups - 1):
                a = aggs[c, h].reshape(piece)
                carried.append(a if h == 0 else gtab[c, 0, h] * carried[h] + a)
            before, behind = zero, zero
            run = None
            for h in range(ngroups - 1, 0, -1):
                here = lows[c, h].reshape(piece) + gtab[c, 1, h] * carried[h]
                run = here if run is None else here + gtab[c, 2, h] * run
                before = jnp.where(gid == h, carried[h], before)
                behind = jnp.where(gid == h - 1, run, behind)
            for i in range(group):
                value = keep[c, i] + tab[c, 2, i] * before + tab[c, 3, i] * behind
                dout[c, i] = value.reshape(dout.shape[2:])
            for o in range(1, group):
                q = lax.rem(mi + o, group)
                send(
                    dout.at[c, q], rbuf.at[c, pl.ds(part_of * nb, nb)],
                    ret_send.at[0], ret_recv.at[c], {"tm": gid * group + q},
                )
            rbuf[c, pl.ds(part_of * nb, nb)] = dout[c, mi]

    squares = jnp.zeros((SUB, LANES), jnp.float32)
    count = len(pairs)
    for n in range(count):
        forward(n)
        send_forcing(n, late[n], fo_recv)
        last_forcing(n)
    for n in range(count):
        send_forcing(n, soon[n], mid_recv)
    ends = [adjoint(n) for n in range(count)]
    for n in range(count):
        finish(n, ends[n])
    for c in range(comps):
        squares = gather(c, squares)
    mine = jnp.sum(squares, axis=0, keepdims=True)
    part_all[flat] = mine
    for o in range(1, across_all):
        other = lax.rem(flat + o, across_all)
        send(
            part_all.at[flat], part_all.at[flat], sum_send.at[0], sum_recv.at[0],
            {"tm": other // space, "space": lax.rem(other, space)},
        )
    for c in range(comps):
        spread(c)

    with mark("sums"):
        all_of(part_all.at[0 : across_all - 1], sum_recv.at[0])
    total = jnp.sum(part_all[...], axis=0)
    entries = across_all * comps * rows * nk * LANES
    rms = jnp.sqrt(jnp.sum(total, axis=(0, 1), keepdims=True) / entries + 1e-06)
    rms_ref[...] = rms
    inverse = jnp.broadcast_to(1.0 / rms, (SUB, LANES))
    for c in range(comps):
        with mark(f"out{c}"):
            with mark(f"out{c}w"):
                all_of(dout.at[c, 0 : group - 1], ret_recv.at[c])
            for k in range(nk):
                for b in range(tiles):
                    at = slice(SUB * b, SUB * (b + 1))
                    out_ref[0, c, at, k * LANES : (k + 1) * LANES] = rbuf[c, k, at] * inverse
    with mark("ends"):
        for d, guard in ((0, has_north), (1, has_south)):
            all_of(cf.at[0 : 3 + comps, :, 0:halo], y_send.at[d], True, guard)
            for n, (c0, c1) in enumerate(pairs):
                sent = late_rows[n] + soon_rows[n]
                all_of(fo.at[c0:c1, 0, :, 0:sent], f_send.at[n, d], True, guard)
        all_of(part.at[0], edge_send.at[0], True, has_prev)
        all_of(nck, edge_send.at[1], True, has_prev)
        all_of(wbuf.at[:, 0 : group - 1], w_send.at[0], True, has_next)
        all_of(wbuf.at[:, 0], w_send.at[1], True, jnp.logical_and(has_next, at_end))
        all_of(gbuf.at[:, 0 : group - 1], g_send.at[0], True)
        for o in range(1, ngroups):
            to = lax.rem(gid + o, ngroups)
            all_of(
                aggs.at[:, 0], agg_send.at[o], True,
                jnp.logical_or(to > gid, gid < ngroups - 1),
            )
            all_of(lows.at[:, 0], low_send.at[o], True, to < gid)
        all_of(dout.at[:, 0 : group - 1], ret_send.at[0], True)
        all_of(part_all.at[0 : across_all - 1], sum_send.at[0], True)


def on_device(tm, space, checkpoint, advect, diffuse, obs_rows, obs_values, obs_weight, error_inverse, rates):
    comps, rows, cols = checkpoint.shape[1:]
    steps, kobs, _, block, _ = obs_values.shape[1:]
    nk = cols // LANES
    tiles = rows // SUB
    group = min(max(tm // 2, 1), nk)
    ngroups = tm // group
    nb = nk // group
    tall = rows + 2 * steps + 2 * SUB
    npairs = len(units_of(comps, steps)[0])
    f32 = jnp.float32
    hbm = pl.BlockSpec(memory_space=pltpu.HBM)
    vmem = pl.BlockSpec(memory_space=pltpu.VMEM)
    dma = pltpu.SemaphoreType.DMA

    def tiled(x):
        lead = x.shape[:-2]
        n = len(lead)
        x = x.reshape(lead + (tiles, SUB, nk, LANES))
        return x.transpose(tuple(range(n)) + (n, n + 2, n + 1, n + 3))

    out, rms = pl.pallas_call(
        functools.partial(kernel, tm, space, group),
        out_shape=(
            pltpu.VMEM((1, comps, rows, cols), f32),
            pltpu.VMEM((1, 1), f32),
        ),
        in_specs=[hbm] * 8,
        out_specs=(vmem, vmem),
        scratch_shapes=[
            pltpu.SMEM((kobs, steps), jnp.int32),
            pltpu.SMEM((1, 1), f32),
            pltpu.SMEM((1, comps), f32),
            pltpu.SMEM((comps, tm), f32),
            pltpu.VMEM((comps, nk, tall, LANES), f32),
            pltpu.VMEM((comps, nk, tall, LANES), f32),
            pltpu.VMEM((2, 3, nk, tall, LANES), f32),
            pltpu.VMEM((2, 3, nk, tall, LANES), f32),
            pltpu.VMEM((comps, 3, nk, tall, LANES), f32),
            pltpu.VMEM((comps, 3, nk, tall, LANES), f32),
            pltpu.VMEM((comps, nk, 2 * SUB, LANES), f32),
            pltpu.VMEM((2, nk, tall, LANES), f32),
            pltpu.VMEM((nk, tall, LANES), f32),
            pltpu.VMEM((7, nk, tall, LANES), f32),
            pltpu.VMEM((steps, kobs, comps, block, cols), f32),
            pltpu.VMEM((comps, steps, nk, tall, LANES), f32),
            pltpu.VMEM((comps, nk, rows, LANES), f32),
            pltpu.VMEM((SUB, LANES), f32),
            pltpu.VMEM((comps, nk, rows, LANES), f32),
            pltpu.VMEM((comps, group, nb, rows, LANES), f32),
            pltpu.VMEM((comps, nk, rows, LANES), f32),
            pltpu.VMEM((comps, group, nb, rows, LANES), f32),
            pltpu.VMEM((comps, group, nb * tiles, SUB, LANES), f32),
            pltpu.VMEM((comps, ngroups, nb, rows, LANES), f32),
            pltpu.VMEM((comps, ngroups, nb, rows, LANES), f32),
            pltpu.VMEM((comps, group, nb, rows, LANES), f32),
            pltpu.VMEM((comps, nk, rows, LANES), f32),
            pltpu.VMEM((comps, 4, group, SUB, LANES), f32),
            pltpu.VMEM((comps, 3, ngroups, SUB, LANES), f32),
            pltpu.VMEM((1, SUB, LANES), f32),
            pltpu.VMEM((tm * space, 1, LANES), f32),
            dma((7 + npairs,)),
            dma((2,)),
            dma((npairs, 2)),
            dma((2,)),
            dma((npairs, 2)),
            dma((npairs, 2)),
            dma((npairs, 2)),
            dma((2,)),
            dma((1 + npairs,)),
            dma((2,)),
            dma((comps, 2)),
            dma((1,)),
            dma((comps,)),
            dma((ngroups,)),
            dma((comps, ngroups)),
            dma((ngroups,)),
            dma((comps, ngroups)),
            dma((1,)),
            dma((comps,)),
            dma((1,)),
            dma((1,)),
        ],
        compiler_params=pltpu.CompilerParams(
            collective_id=0, has_side_effects=True, vmem_limit_bytes=60 * 1024 * 1024
        ),
    )(
        obs_rows[0].T, obs_weight.reshape(1, 1), error_inverse, rates.T,
        tiled(checkpoint[0]), tiled(advect[0]), tiled(diffuse[0]), obs_values[0],
    )
    return out, rms.reshape(())


def solution(mesh):
    placed = (
        P("tm", None, "space", None),
        P("tm", None, "space", None),
        P("tm", "space", None),
        P("tm", None, "space"),
        P("tm", None, "space", None, None, None),
        P("tm"),
        P("tm", None),
        P(),
    )
    return jax.shard_map(
        functools.partial(on_device, mesh.shape["tm"], mesh.shape["space"]),
        mesh=mesh,
        in_specs=placed,
        out_specs=(P("tm", None, "space", None), P()),
        check_vma=False,
    )
```

```python
import functools

import jax
import jax.numpy as jnp
from jax import lax
from jax.experimental import pallas as pl
from jax.experimental.pallas import tpu as pltpu
from jax.sharding import PartitionSpec as P

MESH = pl.DeviceIdType.MESH
LANES = 128
SUB = 8


def mark(name):
    return jax.named_scope(name)


def forcing_spans(first, last):
    spans = []
    while last > first:
        begin = max(last - 2, first)
        spans.append((begin, last, last - first))
        last = begin
    return spans


def units_of(comps, steps):
    units = [(0, 2)] + [(c, c + 1) for c in range(2, comps)]
    return units, [steps // 2] * len(units)


def kernel(
    tm,
    space,
    group,
    rows_hbm,
    weight_hbm,
    einv_hbm,
    rates_hbm,
    ck_hbm,
    adv_hbm,
    dif_hbm,
    obs_hbm,
    out_ref,
    rms_ref,
    rows_smem,
    weight_smem,
    einv_smem,
    rates_smem,
    start,
    fin,
    va,
    vb,
    pa,
    pb,
    mid,
    adv,
    dif,
    cf,
    obs,
    fo,
    nck,
    nei,
    wout,
    wbuf,
    gout,
    gbuf,
    keep,
    aggs,
    lows,
    dout,
    rbuf,
    tab,
    gtab,
    part,
    part_all,
    entered,
    load_sem,
    y_send,
    f_send,
    halo_recv,
    ck_recv,
    fo_recv,
    mid_recv,
    edge_send,
    edge_recv,
    w_send,
    w_recv,
    g_send,
    g_recv,
    agg_send,
    agg_recv,
    low_send,
    low_recv,
    ret_send,
    ret_recv,
    sum_send,
    sum_recv,
):
    comps, tiles, nk = ck_hbm.shape[:3]
    rows = tiles * SUB
    steps, kobs = obs_hbm.shape[:2]
    halo = steps
    lo = SUB
    wide = rows + 2 * halo
    own0 = lo + halo
    ngroups = tm // group
    nb = nk // group
    piece = (nb * tiles, SUB, LANES)
    me = lax.axis_index("tm")
    sp = lax.axis_index("space")
    gid = me // group
    mi = lax.rem(me, group)

    def owner(member, which):
        return member

    part_of = owner(mi, gid)
    own = pl.ds(own0, rows)
    across_all = tm * space
    flat = me * space + sp
    pairs, refetch = units_of(comps, steps)

    def send(src, dst, ssem, rsem, target, guard=None):
        copy = pltpu.make_async_remote_copy(
            src_ref=src, dst_ref=dst, send_sem=ssem, recv_sem=rsem,
            device_id=target, device_id_type=MESH,
        )
        if guard is None:
            copy.start()
        else:
            pl.when(guard)(copy.start)

    def all_of(ref, sem, sent=False, guard=None):
        copy = pltpu.make_async_remote_copy(
            src_ref=ref, dst_ref=ref, send_sem=sem, recv_sem=sem,
            device_id={"tm": lax.rem(me + 1, tm)}, device_id_type=MESH,
        )
        wait = copy.wait_send if sent else copy.wait_recv
        if guard is None:
            wait()
        else:
            pl.when(guard)(wait)

    has_north = sp < space - 1
    has_south = sp > 0
    north = {"space": jnp.minimum(sp + 1, space - 1)}
    south = {"space": jnp.maximum(sp - 1, 0)}
    has_next = me < tm - 1
    has_prev = me > 0
    prv = {"tm": jnp.maximum(me - 1, 0)}

    for b in range(tiles):
        at = pl.ds(own0 + SUB * b, SUB)
        pltpu.make_async_copy(dif_hbm.at[b], dif.at[:, at], load_sem.at[0]).start()
        pltpu.make_async_copy(adv_hbm.at[:, b], adv.at[:, :, at], load_sem.at[1]).start()
        pltpu.make_async_copy(ck_hbm.at[:, b], start.at[:, :, at], load_sem.at[2]).start()
    loads = [
        pltpu.make_async_copy(source, target, load_sem.at[3 + k])
        for k, (source, target) in enumerate(
            [
                (einv_hbm, einv_smem),
                (rates_hbm, rates_smem),
                (rows_hbm, rows_smem),
                (weight_hbm, weight_smem),
            ]
            + [(obs_hbm.at[:, :, c0:c1], obs.at[:, :, c0:c1]) for c0, c1 in pairs]
        )
    ]
    small = 4
    for load in loads:
        load.start()

    barrier = pltpu.get_barrier_semaphore()
    greeters = group - 1 + ngroups - 1
    leads = jnp.logical_and(mi == group - 1, gid < ngroups - 1)

    def greet(sem, target):
        pl.semaphore_signal(sem, inc=1, device_id=target, device_id_type=MESH)

    def greet_peers(sem):
        for o in range(1, group):
            greet(sem, {"tm": gid * group + lax.rem(mi + o, group)})
        for o in range(1, ngroups):
            greet(sem, {"tm": lax.rem(gid + o, ngroups) * group + mi})

    for o in range(1, space):
        greet(barrier, {"space": lax.rem(sp + o, space)})
    greet_peers(barrier)

    @pl.when(leads)
    def _():
        for i in range(group):
            greet(barrier, {"tm": jnp.minimum((gid + 1) * group + i, tm - 1)})

    @pl.when(gid > 0)
    def _():
        greet(barrier, {"tm": jnp.maximum(gid * group - 1, 0)})

    def clear(first):
        blank = jnp.zeros((nk, halo, LANES), jnp.float32)
        at = slice(first, first + halo)
        dif[:, at] = blank
        for a in range(2):
            adv[a, :, at] = blank
        for c in range(comps):
            start[c, :, at] = blank
            for m in range(steps):
                fo[c, m, :, at] = blank
            side = 0 if first < own0 else SUB
            mid[c, :, side : side + SUB] = jnp.zeros((nk, SUB, LANES), jnp.float32)

    @pl.when(jnp.logical_not(has_south))
    def _():
        clear(lo)

    @pl.when(jnp.logical_not(has_north))
    def _():
        clear(own0 + rows)

    @pl.when(jnp.logical_not(has_next))
    def _():
        nck[...] = jnp.zeros_like(nck)
        nei[...] = jnp.zeros_like(nei)

    @pl.when(gid == 0)
    def _():
        for c in range(comps):
            wbuf[c, 0] = jnp.zeros((nb, rows, LANES), jnp.float32)

    with mark("loads"):
        pltpu.make_async_copy(dif.at[:, own], dif.at[:, own], load_sem.at[0]).wait()
        pltpu.make_async_copy(adv.at[:, :, own], adv.at[:, :, own], load_sem.at[1]).wait()
        pltpu.make_async_copy(start.at[:, :, own], start.at[:, :, own], load_sem.at[2]).wait()
        for load in loads[:small]:
            load.wait()
    for c in range(comps):
        part[0, c : c + 1, :] = jnp.full((1, LANES), einv_smem[0, c], jnp.float32)
    with mark("barrier"):
        pl.semaphore_wait(
            barrier,
            greeters + space - 1 + jnp.where(gid > 0, 1, 0) + jnp.where(leads, group, 0),
        )
    greet_peers(entered.at[0])

    def both_ways(lead, ref, depth, ssem, rsem):
        send(
            ref.at[lead + (pl.ds(own0 + rows - depth, depth),)],
            ref.at[lead + (pl.ds(own0 - depth, depth),)],
            ssem.at[0], rsem.at[0], north, has_north,
        )
        send(
            ref.at[lead + (pl.ds(own0, depth),)],
            ref.at[lead + (pl.ds(own0 + rows, depth),)],
            ssem.at[1], rsem.at[1], south, has_south,
        )

    def both_landed(ref, rsem):
        all_of(ref, rsem.at[0], guard=has_south)
        all_of(ref, rsem.at[1], guard=has_north)

    every = slice(None)
    both_ways((every,), dif, halo, y_send, halo_recv)
    both_ways((every, every), adv, halo, y_send, halo_recv)
    send(part.at[0], nei, edge_send.at[0], edge_recv.at[0], prv, has_prev)
    for n, (c0, c1) in enumerate(pairs):
        both_ways((slice(c0, c1), every), start, halo, y_send, ck_recv.at[n])
        send(
            start.at[c0:c1, :, own], nck.at[c0:c1],
            edge_send.at[1], edge_recv.at[1 + n], prv, has_prev,
        )

    def splat(value):
        return jnp.full((SUB, LANES), value, jnp.float32)

    with mark("tables"):
        for c in range(comps):
            keeps, gains = [], []
            for i in range(group):
                r = splat(rates_smem[c, gid * group + i])
                keeps.append(r)
                gains.append(jnp.sqrt(1.0 - r * r))
            after = splat(rates_smem[c, jnp.minimum(gid * group + group, tm - 1)])
            reach = []
            for i in range(group):
                reach.append(keeps[0] if i == 0 else reach[-1] * keeps[i])
            fwd_gain, back_gain = None, after
            for i in range(group - 1, -1, -1):
                if i < group - 1:
                    fwd_gain = gains[i] * reach[i] + keeps[i + 1] * fwd_gain
                    back_gain = keeps[i + 1] * back_gain
                else:
                    fwd_gain = gains[i] * reach[i]
                tab[c, 0, i] = keeps[i]
                tab[c, 1, i] = gains[i]
                tab[c, 2, i] = fwd_gain
                tab[c, 3, i] = back_gain
            for h in range(ngroups):
                total = None
                fwd_gain, back_gain = None, None
                reach = []
                keeps = [splat(rates_smem[c, h * group + i]) for i in range(group)]
                for i in range(group):
                    reach.append(keeps[0] if i == 0 else reach[-1] * keeps[i])
                back_gain = splat(rates_smem[c, min(h * group + group, tm - 1)])
                for i in range(group - 1, -1, -1):
                    here = jnp.sqrt(1.0 - keeps[i] * keeps[i]) * reach[i]
                    if i < group - 1:
                        fwd_gain = here + keeps[i + 1] * fwd_gain
                        back_gain = keeps[i + 1] * back_gain
                    else:
                        fwd_gain = here
                gtab[c, 0, h] = reach[-1]
                gtab[c, 1, h] = fwd_gain
                gtab[c, 2, h] = back_gain

    lane = lax.broadcasted_iota(jnp.int32, (wide, LANES), 1)
    at_first = lane == 0
    at_last = lane == LANES - 1

    def columns(read, dst, at):
        rows_of = at.stop - at.start
        begin, end = at_first[:rows_of], at_last[:rows_of]
        ups, downs = [], []
        for k in range(nk):
            value = read(k)
            ups.append(pltpu.roll(value, LANES - 1, 1))
            downs.append(pltpu.roll(value, 1, 1))
            if k > 0:
                dst[1, k - 1, at] = jnp.where(end, ups[k], ups[k - 1])
                dst[2, k, at] = jnp.where(begin, downs[k - 1], downs[k])
        dst[1, nk - 1, at] = jnp.where(end, ups[0], ups[nk - 1])
        dst[2, 0, at] = jnp.where(begin, downs[nk - 1], downs[0])

    def apply(srcs, k, first, count, adjoint):
        at = slice(first, first + count)
        above = slice(first + 1, first + 1 + count)
        below = slice(first - 1, first - 1 + count)
        if adjoint:
            weights = (cf[0, k, at], cf[5, k, at], cf[6, k, at], cf[4, k, above], cf[3, k, below])
        else:
            weights = (cf[0, k, at], cf[1, k, at], cf[2, k, at], cf[3, k, at], cf[4, k, at])
        return [
            weights[0] * src[0, k, at] + weights[1] * src[1, k, at] + weights[2] * src[2, k, at]
            + weights[3] * src[0, k, above] + weights[4] * src[0, k, below]
            for src in srcs
        ]

    def window(depth):
        pad = -(-2 * depth // SUB) * SUB // 2
        return own0 - pad, rows + 2 * pad

    def step(srcs, dsts, adjoint, adjust, depth, turn):
        first, count = window(depth)
        at = slice(first, first + count)
        begin, end = at_first[:count], at_last[:count]
        ups, downs = {}, {}
        order = [(turn + i) % nk for i in range(nk)]

        def join(west_of, k, n, dst):
            dst[1, west_of, at] = jnp.where(end, ups[k, n], ups[west_of, n])
            dst[2, k, at] = jnp.where(begin, downs[west_of, n], downs[k, n])

        for k in order:
            values = apply(srcs, k, first, count, adjoint)
            for n, dst in enumerate(dsts):
                value = adjust(k, n, at, values[n])
                dst[0, k, at] = value
                ups[k, n] = pltpu.roll(value, LANES - 1, 1)
                downs[k, n] = pltpu.roll(value, 1, 1)
                if k != order[0]:
                    join((k - 1) % nk, k, n, dst)
        for n, dst in enumerate(dsts):
            join(order[-1], order[0], n, dst)

    def beside(source, dst):
        for side, first in ((0, own0 - SUB), (1, own0 + rows)):
            near = slice(first, first + SUB)

            def read(k):
                value = source(side, k, near)
                dst[0, k, near] = value
                return value

            columns(read, dst, near)

    def inside(source, dst):
        mine = slice(own0, own0 + rows)

        def read(k):
            value = source(k, mine)
            dst[0, k, mine] = value
            return value

        columns(read, dst, mine)

    def ready(n):
        c0, c1 = pairs[n]
        for c in range(c0, c1):
            inside(lambda k, mine: start[c, k, mine], va.at[c - c0])

    ready(0)
    with mark("halos"):
        both_landed(cf.at[0:3, :, 0:halo], halo_recv)
    with mark("coefs"):
        at = slice(lo, lo + wide)
        easts, wests = [], []
        for k in range(nk):
            d, a0, a1 = dif[k, at], adv[0, k, at], adv[1, k, at]
            cf[0, k, at] = 1.0 - 4.0 * d
            easts.append(d - 0.5 * a0)
            wests.append(d + 0.5 * a0)
            cf[1, k, at] = easts[k]
            cf[2, k, at] = wests[k]
            cf[3, k, at] = d - 0.5 * a1
            cf[4, k, at] = d + 0.5 * a1
        for k in range(nk):
            up = pltpu.roll(wests[k], LANES - 1, 1)
            cf[5, k, at] = jnp.where(at_last, pltpu.roll(wests[(k + 1) % nk], LANES - 1, 1), up)
            down = pltpu.roll(easts[k], 1, 1)
            cf[6, k, at] = jnp.where(at_first, pltpu.roll(easts[(k - 1) % nk], 1, 1), down)

    weight = weight_smem[0, 0]
    late = [forcing_spans(again, steps - 1) for again in refetch]
    soon = [forcing_spans(0, again - 1) if again > 0 else [] for again in refetch]
    late_rows = [
        sum((last - first) * depth for first, last, depth in spans) + steps - again
        for spans, again in zip(late, refetch)
    ]
    soon_rows = [
        sum((last - first) * depth for first, last, depth in spans) + again
        for spans, again in zip(soon, refetch)
    ]

    def send_forcing(n, spans, rsem):
        c0, c1 = pairs[n]
        for first, last, depth in spans:
            at = pl.ds(first, last - first)
            both_ways((slice(c0, c1), at, every), fo, depth, f_send.at[n], rsem.at[n])

    def forward(n):
        c0, c1 = pairs[n]
        with mark(f"fw{n}"):
            with mark(f"fw{n}w"):
                both_landed(start.at[c0:c1, :, 0:halo], ck_recv.at[n])
                loads[small + n].wait()
            one = [va.at[j] for j in range(c1 - c0)]
            two = [vb.at[j] for j in range(c1 - c0)]
            if n > 0:
                ready(n)
            for c in range(c0, c1):
                beside(lambda side, k, near: start[c, k, near], one[c - c0])

            def watch(t, dsts):
                picks = [
                    [jnp.where(rows_smem[i, t] == b, weight, 0.0) for i in range(kobs)]
                    for b in range(tiles)
                ]

                def compare(k, j, b, value):
                    c = c0 + j
                    lanes = slice(k * LANES, (k + 1) * LANES)
                    total = picks[b][0]
                    pulled = picks[b][0] * obs[t, 0, c, :, lanes]
                    for i in range(1, kobs):
                        total = total + picks[b][i]
                        pulled = pulled + picks[b][i] * obs[t, i, c, :, lanes]
                    r = own0 + SUB * b
                    fo[c, t, k, r : r + SUB] = total * value - pulled

                def adjust(k, j, at, value):
                    for b in range(tiles):
                        r = own0 + SUB * b - at.start
                        if r % SUB == 0:
                            compare(k, j, b, value[r : r + SUB])
                    return value

                def after(at):
                    if (own0 - at.start) % SUB:
                        for k in range(nk):
                            for j, dst in enumerate(dsts):
                                for b in range(tiles):
                                    r = own0 + SUB * b
                                    compare(k, j, b, dst[0, k, r : r + SUB])

                return adjust, after

            def advance(t, srcs, dsts, depth):
                adjust, after = watch(t, dsts)
                step(srcs, dsts, False, adjust, depth, t)
                after(slice(window(depth)[0], None))

            for t in range(steps - 1):
                advance(t, one, two, steps - 1 - t)
                one, two = two, one
            adjust, _ = watch(steps - 1, None)
            own_rows = slice(own0, own0 + rows)
            for k in range(nk):
                for j, value in enumerate(apply(one, k, own0, rows, False)):
                    fin[c0 + j, k, own_rows] = adjust(k, j, own_rows, value)

    far_first = (group - 1, *range(1, group - 1))
    far = jnp.where(mi == group - 1, gid + 1, gid)
    at_end = mi == group - 1

    def last_forcing(n):
        c0, c1 = pairs[n]
        with mark(f"lf{n}"):
            with mark(f"lf{n}w"):
                if n == 0:
                    all_of(nei, edge_recv.at[0], guard=has_next)
                all_of(nck.at[c0:c1], edge_recv.at[1 + n], guard=has_next)
            for c in range(c0, c1):
                scale = jnp.broadcast_to(nei[c : c + 1, :], (rows, LANES))
                for k in range(nk):
                    w = scale * (nck[c, k] - fin[c, k, own])
                    fo[c, steps - 1, k, own] = fo[c, steps - 1, k, own] - w
                    wout[c, k] = w
            both_ways(
                (slice(c0, c1), steps - 1, every), fo, steps - refetch[n],
                f_send.at[n], fo_recv.at[n],
            )
            for c in range(c0, c1):
                for o in range(group):
                    t = lax.rem(mi + 1 + o, group)
                    outside = o == group - 1
                    send(
                        wout.at[c, pl.ds(owner(t, far) * nb, nb)], wbuf.at[c, lax.rem(mi + 1, group)],
                        w_send.at[1 if outside else 0], w_recv.at[c, jnp.where(at_end, 0, 1)],
                        {"tm": jnp.minimum(far * group + t, tm - 1)},
                        jnp.logical_and(has_next, at_end) if outside else has_next,
                    )

                @pl.when(mi < group - 1)
                def _():
                    wbuf[c, lax.rem(mi + 1, group)] = wout[c, pl.ds(part_of * nb, nb)]

                inside(lambda k, mine: fo[c, steps - 1, k, mine], pa.at[c])

    def retreat(n, first, last, target, srcs, spare):
        c0, c1 = pairs[n]

        def force(m):
            return lambda k, j, at, value: value + fo[c0 + j, m, k, at]

        for m in range(last, first - 1, -1):
            step(srcs, spare, True, force(m), m - target, steps - m)
            srcs, spare = spare, srcs
        return srcs

    def adjoint(n):
        c0, c1 = pairs[n]
        again = refetch[n]
        with mark(f"ad{n}"):
            with mark(f"ad{n}w"):
                both_landed(fo.at[c0:c1, 0, :, 0 : late_rows[n]], fo_recv.at[n])
            for c in range(c0, c1):
                beside(lambda side, k, near: fo[c, steps - 1, k, near], pa.at[c])
            ends = [pa.at[c] for c in range(c0, c1)]
            spare = [pb.at[c] for c in range(c0, c1)]
            if again == 0:
                return retreat(n, 0, steps - 2, -1, ends, spare)
            ends = retreat(n, again - 1, steps - 2, again - 1, ends, spare)
            for c, end in zip(range(c0, c1), ends):
                send(
                    end.at[0, :, pl.ds(own0 + rows - again, again)],
                    mid.at[c, :, pl.ds(SUB - again, again)],
                    f_send.at[n, 0], mid_recv.at[n, 0], north, has_north,
                )
                send(
                    end.at[0, :, pl.ds(own0, again)], mid.at[c, :, pl.ds(SUB, again)],
                    f_send.at[n, 1], mid_recv.at[n, 1], south, has_south,
                )
            return ends

    def finish(n, one):
        c0, c1 = pairs[n]
        again = refetch[n]
        with mark(f"af{n}"):
            if again > 0:
                with mark(f"af{n}w"):
                    both_landed(fo.at[c0:c1, 0, :, 0 : soon_rows[n]], mid_recv.at[n])
                for c, end in zip(range(c0, c1), one):
                    beside(lambda side, k, near: mid[c, k, SUB * side : SUB * side + SUB], end)
                first = [va.at[j] for j in range(c1 - c0)]
                other = [vb.at[j] for j in range(c1 - c0)]
                retreat(n, again - 2, again - 2, -1, one, first)
                one = retreat(n, 0, again - 3, -1, first, other)
            scales = [jnp.where(me == 0, einv_smem[0, c], 0.0) for c in range(c0, c1)]
            for k in range(nk):
                values = apply(one, k, own0, rows, True)
                for c, scale, value in zip(range(c0, c1), scales, values):
                    gout[c, k] = value + scale * start[c, k, own]
            for c in range(c0, c1):
                for o in far_first:
                    q = lax.rem(mi + o, group)
                    send(
                        gout.at[c, pl.ds(owner(q, gid) * nb, nb)], gbuf.at[c, mi],
                        g_send.at[0], g_recv.at[c], {"tm": gid * group + q},
                    )
                gbuf[c, mi] = gout[c, pl.ds(part_of * nb, nb)]

    def gather(c, squares):
        with mark(f"ga{c}"):
            with mark(f"ga{c}w"):
                all_of(gbuf.at[c, 0 : group - 1], g_recv.at[c])
                all_of(wbuf.at[c, 0], w_recv.at[c, 0], guard=gid > 0)
                all_of(wbuf.at[c, 0 : group - 1], w_recv.at[c, 1], guard=at_end)
                if group > 2:
                    all_of(
                        wbuf.at[c, 0 : group - 2], w_recv.at[c, 1],
                        guard=jnp.logical_not(at_end),
                    )
            run, ahead = None, []
            for i in range(group):
                g = gbuf[c, i].reshape(piece) + wbuf[c, i].reshape(piece)
                squares = squares + jnp.sum(g * g, axis=0)
                run = tab[c, 1, i] * g if i == 0 else tab[c, 0, i] * run + tab[c, 1, i] * g
                ahead.append(run)
            aggs[c, gid] = run.reshape(aggs.shape[2:])
            for i in range(group - 1, -1, -1):
                here = tab[c, 1, i] * ahead[i]
                run = here if i == group - 1 else here + tab[c, 0, i + 1] * run
                keep[c, i] = run
            lows[c, gid] = run.reshape(lows.shape[2:])
            for o in range(1, ngroups):
                to = lax.rem(gid + o, ngroups)
                target = {"tm": to * group + owner(part_of, to)}
                send(
                    aggs.at[c, gid], aggs.at[c, gid], agg_send.at[o], agg_recv.at[c, o],
                    target, jnp.logical_or(to > gid, gid < ngroups - 1),
                )
                send(
                    lows.at[c, gid], lows.at[c, gid], low_send.at[o], low_recv.at[c, o],
                    target, to < gid,
                )
            return squares


    def spread(c):
        with mark(f"sp{c}"):
            with mark(f"sp{c}w"):
                for o in range(1, ngroups):
                    come = lax.rem(gid + ngroups - o, ngroups)
                    all_of(
                        aggs.at[c, 0], agg_recv.at[c, o],
                        guard=jnp.logical_or(gid > come, come < ngroups - 1),
                    )
                    all_of(lows.at[c, 0], low_recv.at[c, o], guard=gid < come)
            zero = jnp.zeros(piece, jnp.float32)
            carried = [zero]
            for h in range(ngroups - 1):
                a = aggs[c, h].reshape(piece)
                carried.append(a if h == 0 else gtab[c, 0, h] * carried[h] + a)
            before, behind = zero, zero
            run = None
            for h in range(ngroups - 1, 0, -1):
                here = lows[c, h].reshape(piece) + gtab[c, 1, h] * carried[h]
                run = here if run is None else here + gtab[c, 2, h] * run
                before = jnp.where(gid == h, carried[h], before)
                behind = jnp.where(gid == h - 1, run, behind)
            for i in range(group):
                value = keep[c, i] + tab[c, 2, i] * before + tab[c, 3, i] * behind
                dout[c, i] = value.reshape(dout.shape[2:])
            for o in far_first:
                q = lax.rem(mi + o, group)
                send(
                    dout.at[c, q], rbuf.at[c, pl.ds(part_of * nb, nb)],
                    ret_send.at[0], ret_recv.at[c], {"tm": gid * group + q},
                )
            rbuf[c, pl.ds(part_of * nb, nb)] = dout[c, mi]

    squares = jnp.zeros((SUB, LANES), jnp.float32)
    count = len(pairs)
    for n in range(count):
        forward(n)
        send_forcing(n, late[n], fo_recv)
        last_forcing(n)
        send_forcing(n, soon[n], mid_recv)
        if n == 0:
            pl.semaphore_wait(entered.at[0], greeters)
            greet_peers(entered.at[1])
    ends = [adjoint(n) for n in range(count)]
    for n in range(count):
        finish(n, ends[n])
    for c in range(comps):
        squares = gather(c, squares)
    pl.semaphore_wait(entered.at[1], greeters)
    mine = jnp.sum(squares, axis=0, keepdims=True)
    part_all[flat] = mine
    for o in range(1, across_all):
        other = lax.rem(flat + o, across_all)
        send(
            part_all.at[flat], part_all.at[flat], sum_send.at[0], sum_recv.at[0],
            {"tm": other // space, "space": lax.rem(other, space)},
        )
    for c in range(comps):
        spread(c)

    with mark("sums"):
        all_of(part_all.at[0 : across_all - 1], sum_recv.at[0])
    total = jnp.sum(part_all[...], axis=0)
    entries = across_all * comps * rows * nk * LANES
    rms = jnp.sqrt(jnp.sum(total, axis=(0, 1), keepdims=True) / entries + 1e-06)
    rms_ref[...] = rms
    inverse = jnp.broadcast_to(1.0 / rms, (SUB, LANES))
    for c in range(comps):
        with mark(f"out{c}"):
            with mark(f"out{c}w"):
                all_of(dout.at[c, 0 : group - 1], ret_recv.at[c])
            for k in range(nk):
                for b in range(tiles):
                    at = slice(SUB * b, SUB * (b + 1))
                    out_ref[0, c, at, k * LANES : (k + 1) * LANES] = rbuf[c, k, at] * inverse
    with mark("ends"):
        for d, guard in ((0, has_north), (1, has_south)):
            all_of(cf.at[0 : 3 + comps, :, 0:halo], y_send.at[d], True, guard)
            for n, (c0, c1) in enumerate(pairs):
                sent = late_rows[n] + soon_rows[n]
                all_of(fo.at[c0:c1, 0, :, 0:sent], f_send.at[n, d], True, guard)
        all_of(part.at[0], edge_send.at[0], True, has_prev)
        all_of(nck, edge_send.at[1], True, has_prev)
        all_of(wbuf.at[:, 0 : group - 1], w_send.at[0], True, has_next)
        all_of(wbuf.at[:, 0], w_send.at[1], True, jnp.logical_and(has_next, at_end))
        all_of(gbuf.at[:, 0 : group - 1], g_send.at[0], True)
        for o in range(1, ngroups):
            to = lax.rem(gid + o, ngroups)
            all_of(
                aggs.at[:, 0], agg_send.at[o], True,
                jnp.logical_or(to > gid, gid < ngroups - 1),
            )
            all_of(lows.at[:, 0], low_send.at[o], True, to < gid)
        all_of(dout.at[:, 0 : group - 1], ret_send.at[0], True)
        all_of(part_all.at[0 : across_all - 1], sum_send.at[0], True)


def on_device(tm, space, checkpoint, advect, diffuse, obs_rows, obs_values, obs_weight, error_inverse, rates):
    comps, rows, cols = checkpoint.shape[1:]
    steps, kobs, _, block, _ = obs_values.shape[1:]
    nk = cols // LANES
    tiles = rows // SUB
    group = min(max(tm // 2, 1), nk)
    ngroups = tm // group
    nb = nk // group
    tall = rows + 2 * steps + 2 * SUB
    npairs = len(units_of(comps, steps)[0])
    f32 = jnp.float32
    hbm = pl.BlockSpec(memory_space=pltpu.HBM)
    vmem = pl.BlockSpec(memory_space=pltpu.VMEM)
    dma = pltpu.SemaphoreType.DMA

    def tiled(x):
        lead = x.shape[:-2]
        n = len(lead)
        x = x.reshape(lead + (tiles, SUB, nk, LANES))
        return x.transpose(tuple(range(n)) + (n, n + 2, n + 1, n + 3))

    out, rms = pl.pallas_call(
        functools.partial(kernel, tm, space, group),
        out_shape=(
            pltpu.VMEM((1, comps, rows, cols), f32),
            pltpu.VMEM((1, 1), f32),
        ),
        in_specs=[hbm] * 8,
        out_specs=(vmem, vmem),
        scratch_shapes=[
            pltpu.SMEM((kobs, steps), jnp.int32),
            pltpu.SMEM((1, 1), f32),
            pltpu.SMEM((1, comps), f32),
            pltpu.SMEM((comps, tm), f32),
            pltpu.VMEM((comps, nk, tall, LANES), f32),
            pltpu.VMEM((comps, nk, tall, LANES), f32),
            pltpu.VMEM((2, 3, nk, tall, LANES), f32),
            pltpu.VMEM((2, 3, nk, tall, LANES), f32),
            pltpu.VMEM((comps, 3, nk, tall, LANES), f32),
            pltpu.VMEM((comps, 3, nk, tall, LANES), f32),
            pltpu.VMEM((comps, nk, 2 * SUB, LANES), f32),
            pltpu.VMEM((2, nk, tall, LANES), f32),
            pltpu.VMEM((nk, tall, LANES), f32),
            pltpu.VMEM((7, nk, tall, LANES), f32),
            pltpu.VMEM((steps, kobs, comps, block, cols), f32),
            pltpu.VMEM((comps, steps, nk, tall, LANES), f32),
            pltpu.VMEM((comps, nk, rows, LANES), f32),
            pltpu.VMEM((SUB, LANES), f32),
            pltpu.VMEM((comps, nk, rows, LANES), f32),
            pltpu.VMEM((comps, group, nb, rows, LANES), f32),
            pltpu.VMEM((comps, nk, rows, LANES), f32),
            pltpu.VMEM((comps, group, nb, rows, LANES), f32),
            pltpu.VMEM((comps, group, nb * tiles, SUB, LANES), f32),
            pltpu.VMEM((comps, ngroups, nb, rows, LANES), f32),
            pltpu.VMEM((comps, ngroups, nb, rows, LANES), f32),
            pltpu.VMEM((comps, group, nb, rows, LANES), f32),
            pltpu.VMEM((comps, nk, rows, LANES), f32),
            pltpu.VMEM((comps, 4, group, SUB, LANES), f32),
            pltpu.VMEM((comps, 3, ngroups, SUB, LANES), f32),
            pltpu.VMEM((1, SUB, LANES), f32),
            pltpu.VMEM((tm * space, 1, LANES), f32),
            pltpu.SemaphoreType.REGULAR((2,)),
            dma((7 + npairs,)),
            dma((2,)),
            dma((npairs, 2)),
            dma((2,)),
            dma((npairs, 2)),
            dma((npairs, 2)),
            dma((npairs, 2)),
            dma((2,)),
            dma((1 + npairs,)),
            dma((2,)),
            dma((comps, 2)),
            dma((1,)),
            dma((comps,)),
            dma((ngroups,)),
            dma((comps, ngroups)),
            dma((ngroups,)),
            dma((comps, ngroups)),
            dma((1,)),
            dma((comps,)),
            dma((1,)),
            dma((1,)),
        ],
        compiler_params=pltpu.CompilerParams(
            collective_id=0, has_side_effects=True, vmem_limit_bytes=60 * 1024 * 1024
        ),
    )(
        obs_rows[0].T, obs_weight.reshape(1, 1), error_inverse, rates.T,
        tiled(checkpoint[0]), tiled(advect[0]), tiled(diffuse[0]), obs_values[0],
    )
    return out, rms.reshape(())


def solution(mesh):
    placed = (
        P("tm", None, "space", None),
        P("tm", None, "space", None),
        P("tm", "space", None),
        P("tm", None, "space"),
        P("tm", None, "space", None, None, None),
        P("tm"),
        P("tm", None),
        P(),
    )
    return jax.shard_map(
        functools.partial(on_device, mesh.shape["tm"], mesh.shape["space"]),
        mesh=mesh,
        in_specs=placed,
        out_specs=(P("tm", None, "space", None), P()),
        check_vma=False,
    )
```

```python
import functools

import jax
import jax.numpy as jnp
from jax import lax
from jax.experimental import pallas as pl
from jax.experimental.pallas import tpu as pltpu
from jax.sharding import PartitionSpec as P

MESH = pl.DeviceIdType.MESH
LANES = 128
SUB = 8


def mark(name):
    return jax.named_scope(name)


def forcing_spans(first, last):
    spans = []
    while last > first:
        begin = max(last - 2, first)
        spans.append((begin, last, last - first))
        last = begin
    return spans


def units_of(comps, steps):
    units = [(0, 2)] + [(c, c + 1) for c in range(2, comps)]
    return units, [steps // 2] * len(units)


def kernel(
    tm,
    space,
    group,
    rows_hbm,
    weight_hbm,
    einv_hbm,
    rates_hbm,
    ck_hbm,
    adv_hbm,
    dif_hbm,
    obs_hbm,
    out_ref,
    rms_ref,
    rows_smem,
    weight_smem,
    einv_smem,
    rates_smem,
    start,
    fin,
    va,
    vb,
    pa,
    pb,
    mid,
    adv,
    dif,
    cf,
    obs,
    fo,
    nck,
    nei,
    wout,
    wbuf,
    gout,
    gbuf,
    keep,
    aggs,
    lows,
    dout,
    rbuf,
    tab,
    gtab,
    part,
    part_all,
    entered,
    load_sem,
    y_send,
    f_send,
    halo_recv,
    ck_recv,
    fo_recv,
    mid_recv,
    edge_send,
    edge_recv,
    w_send,
    w_recv,
    g_send,
    g_recv,
    agg_send,
    agg_recv,
    low_send,
    low_recv,
    ret_send,
    ret_recv,
    sum_send,
    sum_recv,
):
    comps, tiles, nk = ck_hbm.shape[:3]
    rows = tiles * SUB
    steps, kobs = obs_hbm.shape[:2]
    halo = steps
    lo = SUB
    wide = rows + 2 * halo
    own0 = lo + halo
    ngroups = tm // group
    nb = nk // group
    piece = (nb * tiles, SUB, LANES)
    me = lax.axis_index("tm")
    sp = lax.axis_index("space")
    gid = me // group
    mi = lax.rem(me, group)

    def owner(member, which):
        return member

    part_of = owner(mi, gid)
    own = pl.ds(own0, rows)
    across_all = tm * space
    flat = me * space + sp
    pairs, refetch = units_of(comps, steps)

    def send(src, dst, ssem, rsem, target, guard=None):
        copy = pltpu.make_async_remote_copy(
            src_ref=src, dst_ref=dst, send_sem=ssem, recv_sem=rsem,
            device_id=target, device_id_type=MESH,
        )
        if guard is None:
            copy.start()
        else:
            pl.when(guard)(copy.start)

    def all_of(ref, sem, sent=False, guard=None):
        copy = pltpu.make_async_remote_copy(
            src_ref=ref, dst_ref=ref, send_sem=sem, recv_sem=sem,
            device_id={"tm": lax.rem(me + 1, tm)}, device_id_type=MESH,
        )
        wait = copy.wait_send if sent else copy.wait_recv
        if guard is None:
            wait()
        else:
            pl.when(guard)(wait)

    has_north = sp < space - 1
    has_south = sp > 0
    north = {"space": jnp.minimum(sp + 1, space - 1)}
    south = {"space": jnp.maximum(sp - 1, 0)}
    has_next = me < tm - 1
    has_prev = me > 0
    prv = {"tm": jnp.maximum(me - 1, 0)}

    for b in range(tiles):
        at = pl.ds(own0 + SUB * b, SUB)
        pltpu.make_async_copy(dif_hbm.at[b], dif.at[:, at], load_sem.at[0]).start()
        pltpu.make_async_copy(adv_hbm.at[:, b], adv.at[:, :, at], load_sem.at[1]).start()
        pltpu.make_async_copy(ck_hbm.at[:, b], start.at[:, :, at], load_sem.at[2]).start()
    loads = [
        pltpu.make_async_copy(source, target, load_sem.at[3 + k])
        for k, (source, target) in enumerate(
            [
                (einv_hbm, einv_smem),
                (rates_hbm, rates_smem),
                (rows_hbm, rows_smem),
                (weight_hbm, weight_smem),
            ]
            + [(obs_hbm.at[:, :, c0:c1], obs.at[:, :, c0:c1]) for c0, c1 in pairs]
        )
    ]
    small = 4
    for load in loads:
        load.start()

    barrier = pltpu.get_barrier_semaphore()
    greeters = group - 1 + ngroups - 1
    leads = jnp.logical_and(mi == group - 1, gid < ngroups - 1)

    def greet(sem, target):
        pl.semaphore_signal(sem, inc=1, device_id=target, device_id_type=MESH)

    def greet_peers(sem):
        for o in range(1, group):
            greet(sem, {"tm": gid * group + lax.rem(mi + o, group)})
        for o in range(1, ngroups):
            greet(sem, {"tm": lax.rem(gid + o, ngroups) * group + mi})

    for o in range(1, space):
        greet(barrier, {"space": lax.rem(sp + o, space)})
    greet_peers(barrier)

    @pl.when(leads)
    def _():
        for i in range(group):
            greet(barrier, {"tm": jnp.minimum((gid + 1) * group + i, tm - 1)})

    @pl.when(gid > 0)
    def _():
        greet(barrier, {"tm": jnp.maximum(gid * group - 1, 0)})

    def clear(first):
        blank = jnp.zeros((nk, halo, LANES), jnp.float32)
        at = slice(first, first + halo)
        dif[:, at] = blank
        for a in range(2):
            adv[a, :, at] = blank
        for c in range(comps):
            start[c, :, at] = blank
            for m in range(steps):
                fo[c, m, :, at] = blank
            side = 0 if first < own0 else SUB
            mid[c, :, side : side + SUB] = jnp.zeros((nk, SUB, LANES), jnp.float32)

    @pl.when(jnp.logical_not(has_south))
    def _():
        clear(lo)

    @pl.when(jnp.logical_not(has_north))
    def _():
        clear(own0 + rows)

    @pl.when(jnp.logical_not(has_next))
    def _():
        nck[...] = jnp.zeros_like(nck)
        nei[...] = jnp.zeros_like(nei)

    @pl.when(gid == 0)
    def _():
        for c in range(comps):
            wbuf[c, 0] = jnp.zeros((nb, rows, LANES), jnp.float32)

    with mark("loads"):
        pltpu.make_async_copy(dif.at[:, own], dif.at[:, own], load_sem.at[0]).wait()
        pltpu.make_async_copy(adv.at[:, :, own], adv.at[:, :, own], load_sem.at[1]).wait()
        pltpu.make_async_copy(start.at[:, :, own], start.at[:, :, own], load_sem.at[2]).wait()
        for load in loads[:small]:
            load.wait()
    for c in range(comps):
        part[0, c : c + 1, :] = jnp.full((1, LANES), einv_smem[0, c], jnp.float32)
    with mark("barrier"):
        pl.semaphore_wait(
            barrier,
            greeters + space - 1 + jnp.where(gid > 0, 1, 0) + jnp.where(leads, group, 0),
        )
    greet_peers(entered.at[0])

    def both_ways(lead, ref, depth, ssem, rsem):
        send(
            ref.at[lead + (pl.ds(own0 + rows - depth, depth),)],
            ref.at[lead + (pl.ds(own0 - depth, depth),)],
            ssem.at[0], rsem.at[0], north, has_north,
        )
        send(
            ref.at[lead + (pl.ds(own0, depth),)],
            ref.at[lead + (pl.ds(own0 + rows, depth),)],
            ssem.at[1], rsem.at[1], south, has_south,
        )

    def both_landed(ref, rsem):
        all_of(ref, rsem.at[0], guard=has_south)
        all_of(ref, rsem.at[1], guard=has_north)

    every = slice(None)
    both_ways((every,), dif, halo, y_send, halo_recv)
    both_ways((every, every), adv, halo, y_send, halo_recv)
    send(part.at[0], nei, edge_send.at[0], edge_recv.at[0], prv, has_prev)
    for n, (c0, c1) in enumerate(pairs):
        both_ways((slice(c0, c1), every), start, halo, y_send, ck_recv.at[n])
        send(
            start.at[c0:c1, :, own], nck.at[c0:c1],
            edge_send.at[1], edge_recv.at[1 + n], prv, has_prev,
        )

    def splat(value):
        return jnp.full((SUB, LANES), value, jnp.float32)

    with mark("tables"):
        for c in range(comps):
            keeps, gains = [], []
            for i in range(group):
                r = splat(rates_smem[c, gid * group + i])
                keeps.append(r)
                gains.append(jnp.sqrt(1.0 - r * r))
            after = splat(rates_smem[c, jnp.minimum(gid * group + group, tm - 1)])
            reach = []
            for i in range(group):
                reach.append(keeps[0] if i == 0 else reach[-1] * keeps[i])
            fwd_gain, back_gain = None, after
            for i in range(group - 1, -1, -1):
                if i < group - 1:
                    fwd_gain = gains[i] * reach[i] + keeps[i + 1] * fwd_gain
                    back_gain = keeps[i + 1] * back_gain
                else:
                    fwd_gain = gains[i] * reach[i]
                tab[c, 0, i] = keeps[i]
                tab[c, 1, i] = gains[i]
                tab[c, 2, i] = fwd_gain
                tab[c, 3, i] = back_gain
            for h in range(ngroups):
                total = None
                fwd_gain, back_gain = None, None
                reach = []
                keeps = [splat(rates_smem[c, h * group + i]) for i in range(group)]
                for i in range(group):
                    reach.append(keeps[0] if i == 0 else reach[-1] * keeps[i])
                back_gain = splat(rates_smem[c, min(h * group + group, tm - 1)])
                for i in range(group - 1, -1, -1):
                    here = jnp.sqrt(1.0 - keeps[i] * keeps[i]) * reach[i]
                    if i < group - 1:
                        fwd_gain = here + keeps[i + 1] * fwd_gain
                        back_gain = keeps[i + 1] * back_gain
                    else:
                        fwd_gain = here
                gtab[c, 0, h] = reach[-1]
                gtab[c, 1, h] = fwd_gain
                gtab[c, 2, h] = back_gain

    lane = lax.broadcasted_iota(jnp.int32, (wide, LANES), 1)
    at_first = lane == 0
    at_last = lane == LANES - 1

    def columns(read, dst, at):
        rows_of = at.stop - at.start
        begin, end = at_first[:rows_of], at_last[:rows_of]
        ups, downs = [], []
        for k in range(nk):
            value = read(k)
            ups.append(pltpu.roll(value, LANES - 1, 1))
            downs.append(pltpu.roll(value, 1, 1))
            if k > 0:
                dst[1, k - 1, at] = jnp.where(end, ups[k], ups[k - 1])
                dst[2, k, at] = jnp.where(begin, downs[k - 1], downs[k])
        dst[1, nk - 1, at] = jnp.where(end, ups[0], ups[nk - 1])
        dst[2, 0, at] = jnp.where(begin, downs[nk - 1], downs[0])

    def apply(srcs, k, first, count, adjoint):
        at = slice(first, first + count)
        above = slice(first + 1, first + 1 + count)
        below = slice(first - 1, first - 1 + count)
        if adjoint:
            weights = (cf[0, k, at], cf[5, k, at], cf[6, k, at], cf[4, k, above], cf[3, k, below])
        else:
            weights = (cf[0, k, at], cf[1, k, at], cf[2, k, at], cf[3, k, at], cf[4, k, at])
        return [
            weights[0] * src[0, k, at] + weights[1] * src[1, k, at] + weights[2] * src[2, k, at]
            + weights[3] * src[0, k, above] + weights[4] * src[0, k, below]
            for src in srcs
        ]

    def window(depth):
        pad = -(-2 * depth // SUB) * SUB // 2
        return own0 - pad, rows + 2 * pad

    def step(srcs, dsts, adjoint, adjust, depth, turn):
        first, count = window(depth)
        at = slice(first, first + count)
        begin, end = at_first[:count], at_last[:count]
        ups, downs = {}, {}
        order = [(turn + i) % nk for i in range(nk)]

        def join(west_of, k, n, dst):
            dst[1, west_of, at] = jnp.where(end, ups[k, n], ups[west_of, n])
            dst[2, k, at] = jnp.where(begin, downs[west_of, n], downs[k, n])

        for k in order:
            values = apply(srcs, k, first, count, adjoint)
            for n, dst in enumerate(dsts):
                value = adjust(k, n, at, values[n])
                dst[0, k, at] = value
                ups[k, n] = pltpu.roll(value, LANES - 1, 1)
                downs[k, n] = pltpu.roll(value, 1, 1)
                if k != order[0]:
                    join((k - 1) % nk, k, n, dst)
        for n, dst in enumerate(dsts):
            join(order[-1], order[0], n, dst)

    def beside(source, dst):
        for side, first in ((0, own0 - SUB), (1, own0 + rows)):
            near = slice(first, first + SUB)

            def read(k):
                value = source(side, k, near)
                dst[0, k, near] = value
                return value

            columns(read, dst, near)

    def inside(source, dst):
        mine = slice(own0, own0 + rows)

        def read(k):
            value = source(k, mine)
            dst[0, k, mine] = value
            return value

        columns(read, dst, mine)

    def ready(n):
        c0, c1 = pairs[n]
        for c in range(c0, c1):
            inside(lambda k, mine: start[c, k, mine], va.at[c - c0])

    ready(0)
    with mark("halos"):
        both_landed(cf.at[0:3, :, 0:halo], halo_recv)
    with mark("coefs"):
        at = slice(lo, lo + wide)
        easts, wests = [], []
        for k in range(nk):
            d, a0, a1 = dif[k, at], adv[0, k, at], adv[1, k, at]
            cf[0, k, at] = 1.0 - 4.0 * d
            easts.append(d - 0.5 * a0)
            wests.append(d + 0.5 * a0)
            cf[1, k, at] = easts[k]
            cf[2, k, at] = wests[k]
            cf[3, k, at] = d - 0.5 * a1
            cf[4, k, at] = d + 0.5 * a1
        for k in range(nk):
            up = pltpu.roll(wests[k], LANES - 1, 1)
            cf[5, k, at] = jnp.where(at_last, pltpu.roll(wests[(k + 1) % nk], LANES - 1, 1), up)
            down = pltpu.roll(easts[k], 1, 1)
            cf[6, k, at] = jnp.where(at_first, pltpu.roll(easts[(k - 1) % nk], 1, 1), down)

    weight = weight_smem[0, 0]
    late = [forcing_spans(again, steps - 1) for again in refetch]
    soon = [forcing_spans(0, again - 1) if again > 0 else [] for again in refetch]
    late_rows = [
        sum((last - first) * depth for first, last, depth in spans) + steps - again
        for spans, again in zip(late, refetch)
    ]
    soon_rows = [
        sum((last - first) * depth for first, last, depth in spans) + again
        for spans, again in zip(soon, refetch)
    ]

    def send_forcing(n, spans, rsem):
        c0, c1 = pairs[n]
        for first, last, depth in spans:
            at = pl.ds(first, last - first)
            both_ways((slice(c0, c1), at, every), fo, depth, f_send.at[n], rsem.at[n])

    def forward(n):
        c0, c1 = pairs[n]
        with mark(f"fw{n}"):
            with mark(f"fw{n}w"):
                both_landed(start.at[c0:c1, :, 0:halo], ck_recv.at[n])
                loads[small + n].wait()
            one = [va.at[j] for j in range(c1 - c0)]
            two = [vb.at[j] for j in range(c1 - c0)]
            if n > 0:
                ready(n)
            for c in range(c0, c1):
                beside(lambda side, k, near: start[c, k, near], one[c - c0])

            def watch(t, dsts):
                picks = [
                    [jnp.where(rows_smem[i, t] == b, weight, 0.0) for i in range(kobs)]
                    for b in range(tiles)
                ]

                def compare(k, j, b, value):
                    c = c0 + j
                    lanes = slice(k * LANES, (k + 1) * LANES)
                    total = picks[b][0]
                    pulled = picks[b][0] * obs[t, 0, c, :, lanes]
                    for i in range(1, kobs):
                        total = total + picks[b][i]
                        pulled = pulled + picks[b][i] * obs[t, i, c, :, lanes]
                    r = own0 + SUB * b
                    fo[c, t, k, r : r + SUB] = total * value - pulled

                def adjust(k, j, at, value):
                    for b in range(tiles):
                        r = own0 + SUB * b - at.start
                        if r % SUB == 0:
                            compare(k, j, b, value[r : r + SUB])
                    return value

                def after(at):
                    if (own0 - at.start) % SUB:
                        for k in range(nk):
                            for j, dst in enumerate(dsts):
                                for b in range(tiles):
                                    r = own0 + SUB * b
                                    compare(k, j, b, dst[0, k, r : r + SUB])

                return adjust, after

            def advance(t, srcs, dsts, depth):
                adjust, after = watch(t, dsts)
                step(srcs, dsts, False, adjust, depth, t)
                after(slice(window(depth)[0], None))

            for t in range(steps - 1):
                advance(t, one, two, steps - 1 - t)
                one, two = two, one
            adjust, _ = watch(steps - 1, None)
            own_rows = slice(own0, own0 + rows)
            for k in range(nk):
                for j, value in enumerate(apply(one, k, own0, rows, False)):
                    fin[c0 + j, k, own_rows] = adjust(k, j, own_rows, value)

    far = jnp.where(mi == group - 1, gid + 1, gid)
    at_end = mi == group - 1

    def last_forcing(n):
        c0, c1 = pairs[n]
        with mark(f"lf{n}"):
            with mark(f"lf{n}w"):
                if n == 0:
                    all_of(nei, edge_recv.at[0], guard=has_next)
                all_of(nck.at[c0:c1], edge_recv.at[1 + n], guard=has_next)
            for c in range(c0, c1):
                scale = jnp.broadcast_to(nei[c : c + 1, :], (rows, LANES))
                for k in range(nk):
                    w = scale * (nck[c, k] - fin[c, k, own])
                    fo[c, steps - 1, k, own] = fo[c, steps - 1, k, own] - w
                    wout[c, k] = w
            both_ways(
                (slice(c0, c1), steps - 1, every), fo, steps - refetch[n],
                f_send.at[n], fo_recv.at[n],
            )
            for c in range(c0, c1):
                for o in range(group):
                    t = lax.rem(mi + 1 + o, group)
                    outside = o == group - 1
                    send(
                        wout.at[c, pl.ds(owner(t, far) * nb, nb)], wbuf.at[c, lax.rem(mi + 1, group)],
                        w_send.at[1 if outside else 0], w_recv.at[c, jnp.where(at_end, 0, 1)],
                        {"tm": jnp.minimum(far * group + t, tm - 1)},
                        jnp.logical_and(has_next, at_end) if outside else has_next,
                    )

                @pl.when(mi < group - 1)
                def _():
                    wbuf[c, lax.rem(mi + 1, group)] = wout[c, pl.ds(part_of * nb, nb)]

                inside(lambda k, mine: fo[c, steps - 1, k, mine], pa.at[c])

    def retreat(n, first, last, target, srcs, spare):
        c0, c1 = pairs[n]

        def force(m):
            return lambda k, j, at, value: value + fo[c0 + j, m, k, at]

        for m in range(last, first - 1, -1):
            step(srcs, spare, True, force(m), m - target, steps - m)
            srcs, spare = spare, srcs
        return srcs

    def adjoint(n):
        c0, c1 = pairs[n]
        again = refetch[n]
        with mark(f"ad{n}"):
            with mark(f"ad{n}w"):
                both_landed(fo.at[c0:c1, 0, :, 0 : late_rows[n]], fo_recv.at[n])
            for c in range(c0, c1):
                beside(lambda side, k, near: fo[c, steps - 1, k, near], pa.at[c])
            ends = [pa.at[c] for c in range(c0, c1)]
            spare = [pb.at[c] for c in range(c0, c1)]
            if again == 0:
                return retreat(n, 0, steps - 2, -1, ends, spare)
            ends = retreat(n, again - 1, steps - 2, again - 1, ends, spare)
            for c, end in zip(range(c0, c1), ends):
                send(
                    end.at[0, :, pl.ds(own0 + rows - again, again)],
                    mid.at[c, :, pl.ds(SUB - again, again)],
                    f_send.at[n, 0], mid_recv.at[n, 0], north, has_north,
                )
                send(
                    end.at[0, :, pl.ds(own0, again)], mid.at[c, :, pl.ds(SUB, again)],
                    f_send.at[n, 1], mid_recv.at[n, 1], south, has_south,
                )
            return ends

    def finish(n, one):
        c0, c1 = pairs[n]
        again = refetch[n]
        with mark(f"af{n}"):
            if again > 0:
                with mark(f"af{n}w"):
                    both_landed(fo.at[c0:c1, 0, :, 0 : soon_rows[n]], mid_recv.at[n])
                for c, end in zip(range(c0, c1), one):
                    beside(lambda side, k, near: mid[c, k, SUB * side : SUB * side + SUB], end)
                first = [va.at[j] for j in range(c1 - c0)]
                other = [vb.at[j] for j in range(c1 - c0)]
                retreat(n, again - 2, again - 2, -1, one, first)
                one = retreat(n, 0, again - 3, -1, first, other)
            scales = [jnp.where(me == 0, einv_smem[0, c], 0.0) for c in range(c0, c1)]
            for k in range(nk):
                values = apply(one, k, own0, rows, True)
                for c, scale, value in zip(range(c0, c1), scales, values):
                    gout[c, k] = value + scale * start[c, k, own]
            for c in range(c0, c1):
                for o in range(1, group):
                    q = lax.rem(mi + o, group)
                    send(
                        gout.at[c, pl.ds(owner(q, gid) * nb, nb)], gbuf.at[c, mi],
                        g_send.at[0], g_recv.at[c], {"tm": gid * group + q},
                    )
                gbuf[c, mi] = gout[c, pl.ds(part_of * nb, nb)]

    def gather(c, squares):
        with mark(f"ga{c}"):
            with mark(f"ga{c}w"):
                all_of(gbuf.at[c, 0 : group - 1], g_recv.at[c])
                all_of(wbuf.at[c, 0], w_recv.at[c, 0], guard=gid > 0)
                all_of(wbuf.at[c, 0 : group - 1], w_recv.at[c, 1], guard=at_end)
                if group > 2:
                    all_of(
                        wbuf.at[c, 0 : group - 2], w_recv.at[c, 1],
                        guard=jnp.logical_not(at_end),
                    )
            run, ahead = None, []
            for i in range(group):
                g = gbuf[c, i].reshape(piece) + wbuf[c, i].reshape(piece)
                squares = squares + jnp.sum(g * g, axis=0)
                run = tab[c, 1, i] * g if i == 0 else tab[c, 0, i] * run + tab[c, 1, i] * g
                ahead.append(run)
            aggs[c, gid] = run.reshape(aggs.shape[2:])
            for i in range(group - 1, -1, -1):
                here = tab[c, 1, i] * ahead[i]
                run = here if i == group - 1 else here + tab[c, 0, i + 1] * run
                keep[c, i] = run
            lows[c, gid] = run.reshape(lows.shape[2:])
            for o in range(1, ngroups):
                to = lax.rem(gid + o, ngroups)
                target = {"tm": to * group + owner(part_of, to)}
                send(
                    aggs.at[c, gid], aggs.at[c, gid], agg_send.at[o], agg_recv.at[c, o],
                    target, jnp.logical_or(to > gid, gid < ngroups - 1),
                )
                send(
                    lows.at[c, gid], lows.at[c, gid], low_send.at[o], low_recv.at[c, o],
                    target, to < gid,
                )
            return squares


    def spread(c):
        with mark(f"sp{c}"):
            with mark(f"sp{c}w"):
                for o in range(1, ngroups):
                    come = lax.rem(gid + ngroups - o, ngroups)
                    all_of(
                        aggs.at[c, 0], agg_recv.at[c, o],
                        guard=jnp.logical_or(gid > come, come < ngroups - 1),
                    )
                    all_of(lows.at[c, 0], low_recv.at[c, o], guard=gid < come)
            zero = jnp.zeros(piece, jnp.float32)
            carried = [zero]
            for h in range(ngroups - 1):
                a = aggs[c, h].reshape(piece)
                carried.append(a if h == 0 else gtab[c, 0, h] * carried[h] + a)
            before, behind = zero, zero
            run = None
            for h in range(ngroups - 1, 0, -1):
                here = lows[c, h].reshape(piece) + gtab[c, 1, h] * carried[h]
                run = here if run is None else here + gtab[c, 2, h] * run
                before = jnp.where(gid == h, carried[h], before)
                behind = jnp.where(gid == h - 1, run, behind)
            for i in range(group):
                value = keep[c, i] + tab[c, 2, i] * before + tab[c, 3, i] * behind
                dout[c, i] = value.reshape(dout.shape[2:])
            for o in range(1, group):
                q = lax.rem(mi + o, group)
                send(
                    dout.at[c, q], rbuf.at[c, pl.ds(part_of * nb, nb)],
                    ret_send.at[0], ret_recv.at[c], {"tm": gid * group + q},
                )
            rbuf[c, pl.ds(part_of * nb, nb)] = dout[c, mi]

    squares = jnp.zeros((SUB, LANES), jnp.float32)
    count = len(pairs)
    for n in range(count):
        forward(n)
        send_forcing(n, late[n], fo_recv)
        last_forcing(n)
        send_forcing(n, soon[n], mid_recv)
        if n == 0:
            pl.semaphore_wait(entered.at[0], greeters)
            greet_peers(entered.at[1])
    ends = [adjoint(n) for n in range(count)]
    for n in range(count):
        finish(n, ends[n])
    for c in range(comps):
        squares = gather(c, squares)
    pl.semaphore_wait(entered.at[1], greeters)
    mine = jnp.sum(squares, axis=0, keepdims=True)
    part_all[flat] = mine
    for o in range(1, across_all):
        other = lax.rem(flat + o, across_all)
        send(
            part_all.at[flat], part_all.at[flat], sum_send.at[0], sum_recv.at[0],
            {"tm": other // space, "space": lax.rem(other, space)},
        )
    for c in range(comps):
        spread(c)

    with mark("sums"):
        all_of(part_all.at[0 : across_all - 1], sum_recv.at[0])
    total = jnp.sum(part_all[...], axis=0)
    entries = across_all * comps * rows * nk * LANES
    rms = jnp.sqrt(jnp.sum(total, axis=(0, 1), keepdims=True) / entries + 1e-06)
    rms_ref[...] = rms
    inverse = jnp.broadcast_to(1.0 / rms, (SUB, LANES))
    for c in range(comps):
        with mark(f"out{c}"):
            with mark(f"out{c}w"):
                all_of(dout.at[c, 0 : group - 1], ret_recv.at[c])
            for k in range(nk):
                for b in range(tiles):
                    at = slice(SUB * b, SUB * (b + 1))
                    out_ref[0, c, at, k * LANES : (k + 1) * LANES] = rbuf[c, k, at] * inverse
    with mark("ends"):
        for d, guard in ((0, has_north), (1, has_south)):
            all_of(cf.at[0 : 3 + comps, :, 0:halo], y_send.at[d], True, guard)
            for n, (c0, c1) in enumerate(pairs):
                sent = late_rows[n] + soon_rows[n]
                all_of(fo.at[c0:c1, 0, :, 0:sent], f_send.at[n, d], True, guard)
        all_of(part.at[0], edge_send.at[0], True, has_prev)
        all_of(nck, edge_send.at[1], True, has_prev)
        all_of(wbuf.at[:, 0 : group - 1], w_send.at[0], True, has_next)
        all_of(wbuf.at[:, 0], w_send.at[1], True, jnp.logical_and(has_next, at_end))
        all_of(gbuf.at[:, 0 : group - 1], g_send.at[0], True)
        for o in range(1, ngroups):
            to = lax.rem(gid + o, ngroups)
            all_of(
                aggs.at[:, 0], agg_send.at[o], True,
                jnp.logical_or(to > gid, gid < ngroups - 1),
            )
            all_of(lows.at[:, 0], low_send.at[o], True, to < gid)
        all_of(dout.at[:, 0 : group - 1], ret_send.at[0], True)
        all_of(part_all.at[0 : across_all - 1], sum_send.at[0], True)


def on_device(tm, space, checkpoint, advect, diffuse, obs_rows, obs_values, obs_weight, error_inverse, rates):
    comps, rows, cols = checkpoint.shape[1:]
    steps, kobs, _, block, _ = obs_values.shape[1:]
    nk = cols // LANES
    tiles = rows // SUB
    group = min(max(tm // 2, 1), nk)
    ngroups = tm // group
    nb = nk // group
    tall = rows + 2 * steps + 2 * SUB
    npairs = len(units_of(comps, steps)[0])
    f32 = jnp.float32
    hbm = pl.BlockSpec(memory_space=pltpu.HBM)
    vmem = pl.BlockSpec(memory_space=pltpu.VMEM)
    dma = pltpu.SemaphoreType.DMA

    def tiled(x):
        lead = x.shape[:-2]
        n = len(lead)
        x = x.reshape(lead + (tiles, SUB, nk, LANES))
        return x.transpose(tuple(range(n)) + (n, n + 2, n + 1, n + 3))

    out, rms = pl.pallas_call(
        functools.partial(kernel, tm, space, group),
        out_shape=(
            pltpu.VMEM((1, comps, rows, cols), f32),
            pltpu.VMEM((1, 1), f32),
        ),
        in_specs=[hbm] * 8,
        out_specs=(vmem, vmem),
        scratch_shapes=[
            pltpu.SMEM((kobs, steps), jnp.int32),
            pltpu.SMEM((1, 1), f32),
            pltpu.SMEM((1, comps), f32),
            pltpu.SMEM((comps, tm), f32),
            pltpu.VMEM((comps, nk, tall, LANES), f32),
            pltpu.VMEM((comps, nk, tall, LANES), f32),
            pltpu.VMEM((2, 3, nk, tall, LANES), f32),
            pltpu.VMEM((2, 3, nk, tall, LANES), f32),
            pltpu.VMEM((comps, 3, nk, tall, LANES), f32),
            pltpu.VMEM((comps, 3, nk, tall, LANES), f32),
            pltpu.VMEM((comps, nk, 2 * SUB, LANES), f32),
            pltpu.VMEM((2, nk, tall, LANES), f32),
            pltpu.VMEM((nk, tall, LANES), f32),
            pltpu.VMEM((7, nk, tall, LANES), f32),
            pltpu.VMEM((steps, kobs, comps, block, cols), f32),
            pltpu.VMEM((comps, steps, nk, tall, LANES), f32),
            pltpu.VMEM((comps, nk, rows, LANES), f32),
            pltpu.VMEM((SUB, LANES), f32),
            pltpu.VMEM((comps, nk, rows, LANES), f32),
            pltpu.VMEM((comps, group, nb, rows, LANES), f32),
            pltpu.VMEM((comps, nk, rows, LANES), f32),
            pltpu.VMEM((comps, group, nb, rows, LANES), f32),
            pltpu.VMEM((comps, group, nb * tiles, SUB, LANES), f32),
            pltpu.VMEM((comps, ngroups, nb, rows, LANES), f32),
            pltpu.VMEM((comps, ngroups, nb, rows, LANES), f32),
            pltpu.VMEM((comps, group, nb, rows, LANES), f32),
            pltpu.VMEM((comps, nk, rows, LANES), f32),
            pltpu.VMEM((comps, 4, group, SUB, LANES), f32),
            pltpu.VMEM((comps, 3, ngroups, SUB, LANES), f32),
            pltpu.VMEM((1, SUB, LANES), f32),
            pltpu.VMEM((tm * space, 1, LANES), f32),
            pltpu.SemaphoreType.REGULAR((2,)),
            dma((7 + npairs,)),
            dma((2,)),
            dma((npairs, 2)),
            dma((2,)),
            dma((npairs, 2)),
            dma((npairs, 2)),
            dma((npairs, 2)),
            dma((2,)),
            dma((1 + npairs,)),
            dma((2,)),
            dma((comps, 2)),
            dma((1,)),
            dma((comps,)),
            dma((ngroups,)),
            dma((comps, ngroups)),
            dma((ngroups,)),
            dma((comps, ngroups)),
            dma((1,)),
            dma((comps,)),
            dma((1,)),
            dma((1,)),
        ],
        compiler_params=pltpu.CompilerParams(
            collective_id=0, has_side_effects=True, vmem_limit_bytes=60 * 1024 * 1024
        ),
    )(
        obs_rows[0].T, obs_weight.reshape(1, 1), error_inverse, rates.T,
        tiled(checkpoint[0]), tiled(advect[0]), tiled(diffuse[0]), obs_values[0],
    )
    return out, rms.reshape(())


def solution(mesh):
    placed = (
        P("tm", None, "space", None),
        P("tm", None, "space", None),
        P("tm", "space", None),
        P("tm", None, "space"),
        P("tm", None, "space", None, None, None),
        P("tm"),
        P("tm", None),
        P(),
    )
    return jax.shard_map(
        functools.partial(on_device, mesh.shape["tm"], mesh.shape["space"]),
        mesh=mesh,
        in_specs=placed,
        out_specs=(P("tm", None, "space", None), P()),
        check_vma=False,
    )
```
